32 devices in a mesh: grp: 4 (over z), ctx: 2 (over y), wid: 4 (over x, core).
Axes of the slice: x: 2, y: 2, z: 4, core: 2. Of those that a mesh axis runs over, the one named last changes fastest.
Arguments:
- query: bfloat16 [256, 64, 128], P(None, 'wid'), may hold values from -64 to 64
- keys: bfloat16 [4, 512, 8, 128], P(None, ('grp', 'ctx'), 'wid'), may hold values from -64 to 64
- values: bfloat16 [4, 512, 8, 128], P(None, ('grp', 'ctx'), 'wid'), may hold values from -6 to 6
- lengths: int32 [4, 8], replicated, may hold values from 32 to 64
- query_pos: int32 [256], replicated, may hold values from 128 to 511
- resid: bfloat16 [256, 5120], P('wid', ('grp', 'ctx')), may hold values from -1.1953125 to 1.1953125
- out_weight: bfloat16 [8192, 5120], P('wid', ('grp', 'ctx')), may hold values from -0.0625 to 0.0625
- enc_weight: bfloat16 [5120, 24576], P('wid', ('grp', 'ctx')), may hold values from -0.078125 to 0.078125
- enc_bias: float32 [24576], P(('grp', 'ctx')), may hold values from -3 to 3
- dec_weight: bfloat16 [24576, 5120], P(('grp', 'ctx'), 'wid'), may hold values from -0.078125 to 0.078125
- dec_bias: float32 [5120], P('wid'), may hold values from -3 to 3
Outputs:
- layer_out: bfloat16 [256, 5120], P('wid', ('grp', 'ctx'))
- enc_grad: bfloat16 [5120, 24576], P('wid', ('grp', 'ctx'))
- enc_bias_grad: float32 [24576], P(('grp', 'ctx'))
- dec_grad: bfloat16 [24576, 5120], P(('grp', 'ctx'), 'wid')
- dec_bias_grad: float32 [5120], P('wid')
The draws below stay inside these ranges and needn't reach their ends.
Inputs may be any that keep to these rules, and one draw needn't show every extreme that they name: `lengths`: live slots of a shard are its first ones.
All inputs are finite; a program needn't handle non-finite values.
Results may differ from the reference program's by a relative error of at most 0.024.
Values may be sent and summed in bfloat16 or wider, within the bound.
A program may use at most 128 MiB of HBM per device.

```python
import jax
import jax.numpy as jnp
from jax import lax

D = 5120
QH = 64
KVH = 8
HD = 128
LAT = 24576
SEQS = 4
ROWS_SEQ = 64
SLOTS = 64
GQA = 8
SHARDS = 8
CACHE = 512
ROWS = 256


def query_and_keys(key):
    base = jax.random.fold_in(key, 11)
    key_query, key_keys = jax.random.split(base, 2)
    query = 2.0 * jax.random.normal(key_query, (ROWS, QH, HD), jnp.float32)
    cached = jax.random.normal(key_keys, (SEQS, CACHE, KVH, HD), jnp.float32)
    return (query, cached)


def draw_query(key, part):
    return query_and_keys(key)[0].astype(jnp.bfloat16)


def draw_keys(key, part):
    return query_and_keys(key)[1].astype(jnp.bfloat16)


def plant(result, rng, low, high):
    spot = [jax.random.randint(jax.random.fold_in(rng, axis), (), 0, length) for axis, length in enumerate(result.shape)]
    main_axis = result.shape.index(max(result.shape))
    neighbour = spot[:main_axis] + [(spot[main_axis] + 1) % result.shape[main_axis]] + spot[main_axis + 1:]
    return result.at[tuple(spot)].set(low).at[tuple(neighbour)].set(high)


def block_levels(stream_key, extent, pieces, least, largest):
    loudness, own = 1.0, jax.random.fold_in(stream_key, 6)
    for dim, blocks in pieces:
        steps = jnp.exp(jax.random.uniform(jax.random.fold_in(own, dim), (blocks,), jnp.float32, least / len(pieces), largest / len(pieces)))
        loudness = loudness * jnp.repeat(steps, extent[dim] // blocks).reshape([-1 if axis == dim else 1 for axis in range(len(extent))])
    return loudness


def normal_values(rng, shape, spread, bound, cuts=(), kind=jnp.bfloat16):
    loudness = block_levels(rng, shape, cuts, -0.22, 0.18) if cuts else 1.0
    drawn = jax.random.normal(rng, shape, jnp.float32) * spread * loudness
    return jnp.minimum(jnp.maximum(drawn, -bound), bound).astype(kind)


def setup_inputs(seed: int = 0) -> dict:
    arg_keys = jax.random.split(jax.random.key(seed), 12)
    return {
        "query": draw_query(jax.random.fold_in(arg_keys[11], 71), 0),
        "keys": draw_keys(jax.random.fold_in(arg_keys[11], 71), 0),
        "values": normal_values(arg_keys[2], (SEQS, CACHE, KVH, HD), 1.0, 6.0, ((1, 8), (2, 4))),
        "lengths": plant(jax.random.randint(arg_keys[3], (SEQS, SHARDS), SLOTS // 2, SLOTS + 1), jax.random.fold_in(arg_keys[3], 1), SLOTS // 2, SLOTS).astype(jnp.int32),
        "query_pos": plant(jax.random.randint(arg_keys[4], (ROWS,), SHARDS * SLOTS // 4, SHARDS * SLOTS), jax.random.fold_in(arg_keys[4], 1), SHARDS * SLOTS // 4, (SHARDS * SLOTS) - 1).astype(jnp.int32),
        "resid": normal_values(arg_keys[5], (ROWS, D), 0.2, 1.1953125, ((0, 4), (1, 8))),
        "out_weight": normal_values(arg_keys[6], (QH * HD, D), (QH * HD) ** -0.5, 0.0625, ((0, 4), (1, 8))),
        "enc_weight": normal_values(arg_keys[7], (D, LAT), D ** -0.5, 0.078125, ((0, 4), (1, 8))),
        "enc_bias": normal_values(arg_keys[8], (LAT,), 0.5, 3.0, ((0, 8),), jnp.float32),
        "dec_weight": normal_values(arg_keys[9], (LAT, D), D ** -0.5, 0.078125, ((0, 8), (1, 4))),
        "dec_bias": normal_values(arg_keys[10], (D,), 0.5, 3.0, ((0, 4),), jnp.float32),
    }


def one_sequence(items):
    q_seq, k_seq, v_seq, key_pos, live_slot, row_position = items
    scores = jnp.einsum("rkgd,tkd->krgt", q_seq.astype(jnp.float32), k_seq.astype(jnp.float32),
                        precision=lax.Precision.HIGHEST) * (HD ** -0.5)
    visible = live_slot[None, :] & (key_pos[None, :] <= row_position[:, None])
    visible_mask = visible[None, :, None, :]
    peak = jnp.max(jnp.where(visible_mask, scores, -1e30), axis=-1)
    weights = jnp.where(visible_mask, jnp.exp(scores - peak[..., None]), 0.0)
    weight_sum = jnp.sum(weights, axis=-1)
    weights_low = lax.optimization_barrier(weights.astype(jnp.bfloat16)).astype(jnp.float32)
    weighted = jnp.einsum("krgt,tkd->rkgd", weights_low, v_seq.astype(jnp.float32),
                          precision=lax.Precision.HIGHEST)
    return weighted / jnp.transpose(weight_sum, (1, 0, 2))[..., None]


def reference(query, keys, values, lengths, query_pos, resid, out_weight, enc_weight, enc_bias, dec_weight, dec_bias):
    slot_ids = jnp.arange(SLOTS, dtype=jnp.int32)
    offsets = (jnp.cumsum(lengths, axis=1) - lengths).astype(jnp.int32)
    key_pos = (offsets[:, :, None] + slot_ids[None, None, :]).astype(jnp.int32).reshape(SEQS, CACHE)
    live_slot = (slot_ids[None, None, :] < lengths[:, :, None]).reshape(SEQS, CACHE)
    q_view = query.reshape(SEQS, ROWS_SEQ, KVH, GQA, HD)
    row_position = query_pos.reshape(SEQS, ROWS_SEQ)
    attn = lax.map(one_sequence, (q_view, keys, values, key_pos, live_slot, row_position))
    attention = attn.astype(jnp.bfloat16).reshape(ROWS, QH * HD)
    layer_out = (jnp.dot(attention, out_weight, preferred_element_type=jnp.float32)
                 + resid.astype(jnp.float32)).astype(jnp.bfloat16)
    preact = jnp.dot(layer_out, enc_weight, preferred_element_type=jnp.float32) + enc_bias
    latents = (jax.nn.softplus(4.0 * preact) * 0.25).astype(jnp.bfloat16)
    recon = jnp.dot(latents, dec_weight, preferred_element_type=jnp.float32)
    scaled_error = ((recon + dec_bias - layer_out.astype(jnp.float32)) * (ROWS ** -0.5)).astype(jnp.bfloat16)
    dec_grad = lax.dot_general(latents, scaled_error, (((0,), (0,)), ((), ())),
                               preferred_element_type=jnp.float32).astype(jnp.bfloat16)
    dec_bias_grad = jnp.sum(scaled_error.astype(jnp.float32), axis=0)
    latent_grad = lax.dot_general(scaled_error, dec_weight, (((1,), (1,)), ((), ())),
                                  preferred_element_type=jnp.float32)
    preact_grad = (latent_grad * jax.nn.sigmoid(4.0 * preact)).astype(jnp.bfloat16)
    enc_grad = lax.dot_general(layer_out, preact_grad, (((0,), (0,)), ((), ())),
                               preferred_element_type=jnp.float32).astype(jnp.bfloat16)
    enc_bias_grad = jnp.sum(preact_grad.astype(jnp.float32), axis=0)
    return layer_out, enc_grad, enc_bias_grad, dec_grad, dec_bias_grad
```

```python
import functools

import jax
import jax.numpy as jnp
from jax import lax
from jax.experimental import pallas as pl
from jax.experimental.pallas import tpu as pltpu
from jax.sharding import PartitionSpec as P

HD = 128
MESH = pl.DeviceIdType.MESH


def exchange_kernel(n, where, peer_id, gather, x_ref, out_ref, send_sem, recv_sem):
    me = where()
    peers = [lax.rem(me + step, n) for step in range(1, n)]
    barrier = pltpu.get_barrier_semaphore()
    for peer in peers:
        pl.semaphore_signal(barrier, inc=1, device_id=peer_id(peer), device_id_type=MESH)
    pl.semaphore_wait(barrier, n - 1)

    def copy_to(step, peer):
        return pltpu.make_async_remote_copy(
            src_ref=x_ref if gather else x_ref.at[peer],
            dst_ref=out_ref.at[me],
            send_sem=send_sem.at[step],
            recv_sem=recv_sem.at[me],
            device_id=peer_id(peer),
            device_id_type=MESH,
        )

    def copy_from(step, peer):
        return pltpu.make_async_remote_copy(
            src_ref=x_ref if gather else x_ref.at[peer],
            dst_ref=out_ref.at[peer],
            send_sem=send_sem.at[step],
            recv_sem=recv_sem.at[peer],
            device_id=peer_id(peer),
            device_id_type=MESH,
        )

    sends = [copy_to(step, peer) for step, peer in enumerate(peers)]
    for copy in sends:
        copy.start()
    out_ref[me] = x_ref[...] if gather else x_ref[me]
    for step, peer in enumerate(peers):
        copy_from(step, peer).wait_recv()
    for copy in sends:
        copy.wait_send()


def exchange(x, n, where, peer_id, gather, number):
    block = x.shape if gather else x.shape[1:]
    return pl.pallas_call(
        functools.partial(exchange_kernel, n, where, peer_id, gather),
        out_shape=jax.ShapeDtypeStruct((n,) + block, x.dtype),
        in_specs=[pl.BlockSpec(memory_space=pltpu.VMEM)],
        out_specs=pl.BlockSpec(memory_space=pltpu.VMEM),
        scratch_shapes=[pltpu.SemaphoreType.DMA((n,)), pltpu.SemaphoreType.DMA((n,))],
        compiler_params=pltpu.CompilerParams(
            collective_id=number, has_side_effects=True, vmem_limit_bytes=24 * 1024 * 1024
        ),
        name="exchange%d" % number,
    )(x)


class Groups:
    def __init__(self, sizes):
        ctx_n = sizes["ctx"]
        self.shards = (
            sizes["grp"] * ctx_n,
            lambda: lax.axis_index("grp") * ctx_n + lax.axis_index("ctx"),
            lambda p: {"grp": p // ctx_n, "ctx": lax.rem(p, ctx_n)},
        )
        self.wid = (sizes["wid"], lambda: lax.axis_index("wid"), lambda p: {"wid": p})
        self.low = (
            2,
            lambda: lax.rem(lax.axis_index("wid"), 2),
            lambda p: {"wid": (lax.axis_index("wid") // 2) * 2 + p},
        )
        self.high = (
            sizes["wid"] // 2,
            lambda: lax.axis_index("wid") // 2,
            lambda p: {"wid": p * 2 + lax.rem(lax.axis_index("wid"), 2)},
        )


def scatter_sum(x, group, number):
    n = group[0]
    parts = exchange(x.reshape((n, x.shape[0] // n) + x.shape[1:]), *group, False, number)
    return jnp.sum(parts.astype(jnp.float32), axis=0)


def gather_rows(x, group, number):
    whole = exchange(x, *group, True, number)
    return whole.reshape((whole.shape[0] * whole.shape[1],) + whole.shape[2:])


def local_copy(src, dst, sem):
    return pltpu.make_async_copy(src, dst, sem)


def rows_at(start, size):
    return pl.ds(pl.multiple_of(start, 16), size)


class Plan:
    def __init__(self, sizes, row_count, width, latents):
        self.grp, self.ctx, self.wid = sizes["grp"], sizes["ctx"], sizes["wid"]
        self.high = self.wid // 2
        self.row_count, self.width, self.latents = row_count, width, latents
        self.streams = 2
        self.rows = row_count // self.streams
        self.half = self.rows // 2
        self.quarter = self.rows // self.wid
        self.side = self.rows // self.ctx
        self.piece = self.side // self.grp

    def fits(self):
        return (
            self.wid % 2 == 0
            and self.row_count % self.streams == 0
            and self.rows % (16 * self.wid) == 0
            and self.rows % (16 * self.grp * self.ctx) == 0
            and self.width % 256 == 0
            and self.latents % 512 == 0
        )


def middle_kernel(
    plan, block, enc_bias, dec_bias, enc_hbm, dec_hbm, lat, err, pgrad,
    enc_w, dec_w, part, pair_in, pair_sum, high_in, factor, recon, side_in, side_sum, piece_in,
    load_sem, pair_sem, high_sem, gather_sem, relay_sem, side_sem, piece_sem, spread_sem, cross_sem,
):
    p = plan
    g, c, w = lax.axis_index("grp"), lax.axis_index("ctx"), lax.axis_index("wid")
    low, high = lax.rem(w, 2), w // 2
    partner = {"wid": w + 1 - 2 * low}
    highs = [lax.rem(high + s, p.high) for s in range(1, p.high)]
    ctxs = [lax.rem(c + s, p.ctx) for s in range(1, p.ctx)]
    grps = [lax.rem(g + s, p.grp) for s in range(1, p.grp)]
    highs_from = [lax.rem(high + p.high - s, p.high) for s in range(1, p.high)]
    grps_from = [lax.rem(g + p.grp - s, p.grp) for s in range(1, p.grp)]
    to_high = lambda h: {"wid": h * 2 + low}
    to_ctx = lambda q: {"ctx": q}
    to_grp = lambda q: {"grp": q}
    peers = [partner] + [to_high(h) for h in highs] + [to_ctx(q) for q in ctxs] + [to_grp(q) for q in grps]

    lat_step = 512
    enc_steps = p.latents // lat_step
    dec_rows = p.latents // 2
    loads = [
        local_copy(enc_hbm.at[:, pl.ds(j * lat_step, lat_step)], enc_w.at[:, pl.ds(j * lat_step, lat_step)], load_sem.at[j])
        for j in range(enc_steps)
    ]
    late_loads = [
        local_copy(dec_hbm.at[pl.ds(j * dec_rows, dec_rows)], dec_w.at[pl.ds(j * dec_rows, dec_rows)], load_sem.at[enc_steps + j])
        for j in range(2)
    ]
    for copy in loads + late_loads:
        copy.start()
    barrier = pltpu.get_barrier_semaphore()
    for peer in peers:
        pl.semaphore_signal(barrier, inc=1, device_id=peer, device_id_type=MESH)
    pl.semaphore_wait(barrier, len(peers))

    pending = []

    def send(src, dst, sem, index, peer):
        copy = pltpu.make_async_remote_copy(
            src_ref=src, dst_ref=dst, send_sem=sem.at[(0,) + index], recv_sem=sem.at[(1,) + index],
            device_id=peer, device_id_type=MESH,
        )
        copy.start()
        pending.append(copy)

    def arrived(ref, sem, index, peer):
        pltpu.make_async_remote_copy(
            src_ref=ref, dst_ref=ref, send_sem=sem.at[(0,) + index], recv_sem=sem.at[(1,) + index],
            device_id=peer, device_id_type=MESH,
        ).wait_recv()

    def quarter_row(t, lo, hi):
        return t * p.rows + (lo * p.high + hi) * p.quarter

    def piece_row(t, q, r):
        return t * p.rows + q * p.side + r * p.piece

    def pair_send(k, t):
        there = part.at[k, rows_at(t * p.rows + (1 - low) * p.half, p.half)]
        send(there, pair_in.at[k, t], pair_sem, (k, t), partner)

    def pair_add(k, t):
        arrived(pair_in.at[k, t], pair_sem, (k, t), partner)

        def step(i, carry):
            r = pl.multiple_of(i * 16, 16)
            mine = part[k, rows_at(t * p.rows + low * p.half + r, 16)].astype(jnp.float32)
            theirs = pair_in[k, t, pl.ds(r, 16)].astype(jnp.float32)
            pair_sum[k, t, pl.ds(r, 16)] = (mine + theirs).astype(jnp.bfloat16)
            return carry

        lax.fori_loop(0, p.half // 16, step, 0)
        for s, h in enumerate(highs):
            send(pair_sum.at[k, t, rows_at(h * p.quarter, p.quarter)], high_in.at[k, t, s], high_sem, (k, t, s), to_high(h))

    def high_sum(k, t, r):
        total = pair_sum[k, t, rows_at(high * p.quarter + r, 16)].astype(jnp.float32)
        for s in range(len(highs)):
            total = total + high_in[k, t, s, pl.ds(r, 16)].astype(jnp.float32)
        return total

    def publish(k, t, out):
        mine = out.at[rows_at(quarter_row(t, low, high), p.quarter)]
        for s, h in enumerate(highs):
            send(mine, mine, gather_sem, (k, t, s + 1), to_high(h))
        send(mine, mine, gather_sem, (k, t, 0), partner)

    def activate(t):
        for s, h in enumerate(highs):
            arrived(high_in.at[0, t, s], high_sem, (0, t, s), to_high(h))

        def step(i, carry):
            r = pl.multiple_of(i * 16, 16)
            z = 4.0 * (high_sum(0, t, r) + enc_bias[...])
            e = jnp.exp(-jnp.abs(z))
            lat[rows_at(quarter_row(t, low, high) + r, 16)] = (
                (jnp.maximum(z, 0.0) + jnp.log1p(e)) * 0.25
            ).astype(jnp.bfloat16)
            factor[t, pl.ds(r, 16)] = jnp.where(z >= 0.0, 1.0, e) / (1.0 + e)
            return carry

        lax.fori_loop(0, p.quarter // 16, step, 0)
        publish(0, t, lat)

    def cotangent(t):
        for s, h in enumerate(highs):
            arrived(high_in.at[1, t, s], high_sem, (1, t, s), to_high(h))

        def step(i, carry):
            r = pl.multiple_of(i * 16, 16)
            pgrad[rows_at(quarter_row(t, low, high) + r, 16)] = (
                high_sum(1, t, r) * factor[t, pl.ds(r, 16)]
            ).astype(jnp.bfloat16)
            return carry

        lax.fori_loop(0, p.quarter // 16, step, 0)
        publish(1, t, pgrad)

    def relay(k, t, out):
        for s, h in enumerate(highs_from):
            theirs = out.at[rows_at(quarter_row(t, low, h), p.quarter)]
            arrived(theirs, gather_sem, (k, t, s + 1), to_high(h))
            send(theirs, theirs, relay_sem, (k, t, s), partner)

    def collected(k, t, out):
        arrived(out.at[rows_at(quarter_row(t, 1 - low, high), p.quarter)], gather_sem, (k, t, 0), partner)
        for s, h in enumerate(highs):
            arrived(out.at[rows_at(quarter_row(t, 1 - low, h), p.quarter)], relay_sem, (k, t, s), partner)

    def encode(t):
        rows = pl.ds(t * p.rows, p.rows)
        for j in range(enc_steps):
            if t == 0:
                loads[j].wait()
            cols = pl.ds(j * lat_step, lat_step)
            part[0, rows, cols] = jnp.dot(
                block[rows, :], enc_w[:, cols], preferred_element_type=jnp.float32
            ).astype(jnp.bfloat16)
        pair_send(0, t)

    def decode(t):
        collected(0, t, lat)
        if t == 0:
            for copy in late_loads:
                copy.wait()
        rows = pl.ds(t * p.rows, p.rows)

        def step(j, carry):
            cols = pl.ds(pl.multiple_of(j * 256, 256), 256)
            recon[rows, cols] = jnp.dot(
                lat[rows, :], dec_w[:, cols], preferred_element_type=jnp.float32
            ).astype(jnp.bfloat16)
            return carry

        lax.fori_loop(0, p.width // 256, step, 0)
        for s, q in enumerate(ctxs):
            send(recon.at[rows_at(piece_row(t, q, 0), p.side)], side_in.at[t, s], side_sem, (t, s), to_ctx(q))

    def side_add(t):
        for s, q in enumerate(ctxs):
            arrived(side_in.at[t, s], side_sem, (t, s), to_ctx(q))

        def step(i, carry):
            r = pl.multiple_of(i * 16, 16)
            total = recon[rows_at(piece_row(t, c, 0) + r, 16)].astype(jnp.float32)
            for s in range(len(ctxs)):
                total = total + side_in[t, s, pl.ds(r, 16)].astype(jnp.float32)
            side_sum[t, pl.ds(r, 16)] = total.astype(jnp.bfloat16)
            return carry

        lax.fori_loop(0, p.side // 16, step, 0)
        for s, q in enumerate(grps):
            send(side_sum.at[t, rows_at(q * p.piece, p.piece)], piece_in.at[t, s], piece_sem, (t, s), to_grp(q))

    def error(t):
        for s, q in enumerate(grps):
            arrived(piece_in.at[t, s], piece_sem, (t, s), to_grp(q))

        def step(i, carry):
            r = pl.multiple_of(i * 16, 16)
            total = side_sum[t, rows_at(g * p.piece + r, 16)].astype(jnp.float32)
            for s in range(len(grps)):
                total = total + piece_in[t, s, pl.ds(r, 16)].astype(jnp.float32)
            rows = rows_at(piece_row(t, c, g) + r, 16)
            wanted = block[rows].astype(jnp.float32)
            err[rows] = ((total + dec_bias[...] - wanted) * p.row_count ** (-0.5)).astype(jnp.bfloat16)
            return carry

        lax.fori_loop(0, p.piece // 16, step, 0)
        mine = err.at[rows_at(piece_row(t, c, g), p.piece)]
        for s, q in enumerate(grps):
            send(mine, mine, spread_sem, (t, s), to_grp(q))
        for s, q in enumerate(ctxs):
            send(mine, mine, cross_sem, (t, s, 0), to_ctx(q))

    def error_relay(t):
        for i, r in enumerate(grps_from):
            theirs = err.at[rows_at(piece_row(t, c, r), p.piece)]
            arrived(theirs, spread_sem, (t, i), to_grp(r))
            for s, q in enumerate(ctxs):
                send(theirs, theirs, cross_sem, (t, s, i + 1), to_ctx(q))

    def back(t):
        for s, q in enumerate(ctxs):
            for i, r in enumerate([g] + grps):
                arrived(err.at[rows_at(piece_row(t, q, r), p.piece)], cross_sem, (t, s, i), to_ctx(q))
        rows = pl.ds(t * p.rows, p.rows)

        def step(j, carry):
            cols = pl.ds(pl.multiple_of(j * lat_step, lat_step), lat_step)
            part[1, rows, cols] = lax.dot_general(
                err[rows, :], dec_w[cols, :], (((1,), (1,)), ((), ())), preferred_element_type=jnp.float32
            ).astype(jnp.bfloat16)
            return carry

        lax.fori_loop(0, enc_steps, step, 0)
        pair_send(1, t)

    stages = [
        lambda: encode(0),
        lambda: encode(1),
        lambda: pair_add(0, 0),
        lambda: pair_add(0, 1),
        lambda: activate(0),
        lambda: activate(1),
        lambda: relay(0, 0, lat),
        lambda: decode(0),
        lambda: relay(0, 1, lat),
        lambda: decode(1),
        lambda: side_add(0),
        lambda: side_add(1),
        lambda: error(0),
        lambda: error(1),
        lambda: error_relay(0),
        lambda: back(0),
        lambda: error_relay(1),
        lambda: pair_add(1, 0),
        lambda: back(1),
        lambda: pair_add(1, 1),
        lambda: cotangent(0),
        lambda: cotangent(1),
        lambda: relay(1, 0, pgrad),
        lambda: relay(1, 1, pgrad),
        lambda: collected(1, 0, pgrad),
        lambda: collected(1, 1, pgrad),
    ]
    for stage in stages:
        stage()
    for copy in pending:
        copy.wait_send()


def middle(plan, block, enc_weight, enc_bias, dec_weight, dec_bias, number):
    p = plan
    low = jnp.bfloat16
    vmem = pl.BlockSpec(memory_space=pltpu.VMEM)
    hbm = pl.BlockSpec(memory_space=pl.ANY)
    n, highs, ctxs, grps = p.streams, p.high - 1, p.ctx - 1, p.grp - 1
    dma = pltpu.SemaphoreType.DMA
    return pl.pallas_call(
        functools.partial(middle_kernel, p),
        out_shape=(
            jax.ShapeDtypeStruct((p.row_count, p.latents), low),
            jax.ShapeDtypeStruct((p.row_count, p.width), low),
            jax.ShapeDtypeStruct((p.row_count, p.latents), low),
        ),
        in_specs=[vmem, vmem, vmem, hbm, hbm],
        out_specs=(vmem, vmem, vmem),
        scratch_shapes=[
            pltpu.VMEM((p.width, p.latents), low),
            pltpu.VMEM((p.latents, p.width), low),
            pltpu.VMEM((2, p.row_count, p.latents), low),
            pltpu.VMEM((2, n, p.half, p.latents), low),
            pltpu.VMEM((2, n, p.half, p.latents), low),
            pltpu.VMEM((2, n, highs, p.quarter, p.latents), low),
            pltpu.VMEM((n, p.quarter, p.latents), jnp.float32),
            pltpu.VMEM((p.row_count, p.width), low),
            pltpu.VMEM((n, ctxs, p.side, p.width), low),
            pltpu.VMEM((n, p.side, p.width), low),
            pltpu.VMEM((n, grps, p.piece, p.width), low),
            dma((p.latents // 512 + 2,)),
            dma((2, 2, n)),
            dma((2, 2, n, highs)),
            dma((2, 2, n, highs + 1)),
            dma((2, 2, n, highs)),
            dma((2, n, ctxs)),
            dma((2, n, grps)),
            dma((2, n, grps)),
            dma((2, n, ctxs, grps + 1)),
        ],
        compiler_params=pltpu.CompilerParams(
            collective_id=number, has_side_effects=True, vmem_limit_bytes=60 * 1024 * 1024
        ),
        name="middle",
    )(block, enc_bias.reshape(1, -1), dec_bias.reshape(1, -1), enc_weight, dec_weight)


def outer_kernel(x_ref, y_ref, out_ref, sum_ref):
    @pl.when(pl.program_id(0) == 0)
    def _():
        sum_ref[...] = jnp.sum(y_ref[...].astype(jnp.float32), axis=0, keepdims=True)

    out_ref[...] = lax.dot_general(
        x_ref[...], y_ref[...], (((0,), (0,)), ((), ())), preferred_element_type=jnp.float32
    ).astype(out_ref.dtype)


def outer(x, y, step, name):
    rows, m = x.shape
    n = y.shape[1]
    out, total = pl.pallas_call(
        outer_kernel,
        grid=(m // step,),
        in_specs=[pl.BlockSpec((rows, step), lambda i: (0, i)), pl.BlockSpec((rows, n), lambda i: (0, 0))],
        out_specs=(pl.BlockSpec((step, n), lambda i: (i, 0)), pl.BlockSpec((1, n), lambda i: (0, 0))),
        out_shape=(jax.ShapeDtypeStruct((m, n), jnp.bfloat16), jax.ShapeDtypeStruct((1, n), jnp.float32)),
        compiler_params=pltpu.CompilerParams(vmem_limit_bytes=32 * 1024 * 1024),
        name=name,
    )(x, y)
    return out, total.reshape(n)


def attend(groups, query, keys, values, lengths, query_pos):
    seq_count, slot_count, kv_local, head_dim = keys.shape
    row_count, heads_local = query.shape[:2]
    group_size = heads_local // kv_local
    shards = groups.shards[0]
    pairs = seq_count * kv_local
    chunks = shards // pairs
    rows = row_count // seq_count // chunks
    pair = lax.axis_index(("grp", "ctx")) // chunks
    seq, head = pair // kv_local, lax.rem(pair, kv_local)
    row0 = seq * (row_count // seq_count) + lax.rem(lax.axis_index(("grp", "ctx")), chunks) * rows
    cache = jnp.concatenate([keys, values], axis=-1).transpose(0, 2, 1, 3)
    cache = cache.reshape(pairs, slot_count, 2 * head_dim)
    if chunks > 1:
        cache = jnp.repeat(cache, chunks, axis=0)
    cache = exchange(cache, *groups.shards, False, 0).reshape(shards * slot_count, 2 * head_dim)
    q = lax.dynamic_slice(query, (row0, head * group_size, 0), (rows, group_size, head_dim))
    live = lax.dynamic_index_in_dim(lengths, seq, 0, keepdims=False)
    before = jnp.arange(shards)[None, :] < jnp.arange(shards)[:, None]
    offset = jnp.sum(jnp.where(before, live[None, :], 0), axis=1)
    slot_ids = jnp.arange(slot_count, dtype=jnp.int32)
    key_pos = jnp.where(
        slot_ids[None, :] < live[:, None], offset[:, None] + slot_ids[None, :], jnp.int32(2**30)
    ).reshape(-1)
    position = lax.dynamic_slice_in_dim(query_pos, row0, rows, 0)
    visible = (key_pos[None, :] <= position[:, None])[:, None, :]
    scores = jnp.einsum(
        "rgd,td->rgt", q, cache[:, :head_dim], preferred_element_type=jnp.float32
    ) * HD ** (-0.5)
    peak = jnp.max(jnp.where(visible, scores, -1e30), axis=-1, keepdims=True)
    weights = jnp.where(visible, jnp.exp(scores - peak), 0.0)
    weight_sum = jnp.sum(weights, axis=-1, keepdims=True)
    weighted = jnp.einsum(
        "rgt,td->rgd", weights.astype(jnp.bfloat16), cache[:, head_dim:],
        preferred_element_type=jnp.float32,
    )
    mine = (weighted / weight_sum).astype(jnp.bfloat16).reshape(rows, group_size * head_dim)
    attention = exchange(mine, *groups.shards, True, 1)
    attention = attention.reshape(seq_count, kv_local, chunks, rows, group_size * head_dim)
    return attention.transpose(0, 2, 3, 1, 4).reshape(row_count, heads_local * head_dim)


def body(
    sizes,
    query,
    keys,
    values,
    lengths,
    query_pos,
    resid,
    out_weight,
    enc_weight,
    enc_bias,
    dec_weight,
    dec_bias,
):
    groups = Groups(sizes)
    row_count = query.shape[0]
    shard_pos = lax.axis_index(("grp", "ctx"))
    attention = attend(groups, query, keys, values, lengths, query_pos)
    projected = jnp.dot(attention, out_weight, preferred_element_type=jnp.float32)
    mixed = scatter_sum(projected.astype(jnp.bfloat16), groups.wid, 2)
    layer_out = (mixed + resid.astype(jnp.float32)).astype(jnp.bfloat16)
    rows, cols = layer_out.shape
    wid_n = sizes["wid"]
    wide = exchange(layer_out, *groups.shards, True, 3)
    wide = wide.reshape(wid_n, -1, rows, cols).transpose(0, 2, 1, 3).reshape(wid_n, rows, -1)
    block = exchange(wide, *groups.wid, False, 4).reshape(row_count, -1)
    plan = Plan(sizes, row_count, block.shape[1], enc_weight.shape[1])
    if plan.fits():
        latents, error_all, preact_grad = middle(
            plan, block, enc_weight, enc_bias, dec_weight, dec_bias, 5
        )
        dec_grad, dec_bias_grad = outer(latents, error_all, 256, "dec_outer")
        enc_grad, enc_bias_grad = outer(block, preact_grad, 128, "enc_outer")
        return (layer_out, enc_grad, enc_bias_grad, dec_grad, dec_bias_grad)
    enc_part = jnp.dot(block, enc_weight, preferred_element_type=jnp.float32)
    preact = scatter_sum(enc_part.astype(jnp.bfloat16), groups.low, 5).astype(jnp.bfloat16)
    preact = scatter_sum(preact, groups.high, 6) + enc_bias
    my_latents = (jax.nn.softplus(4.0 * preact) * 0.25).astype(jnp.bfloat16)
    latents = gather_rows(gather_rows(my_latents, groups.high, 7), groups.low, 8)
    row_scale = row_count ** (-0.5)
    recon = jnp.dot(latents, dec_weight, preferred_element_type=jnp.float32)
    recon = scatter_sum(recon.astype(jnp.bfloat16), groups.shards, 9)
    piece_len = recon.shape[0]
    target = lax.dynamic_slice_in_dim(block, shard_pos * piece_len, piece_len, 0).astype(
        jnp.float32
    )
    scaled_error = ((recon + dec_bias - target) * row_scale).astype(jnp.bfloat16)
    error_all = gather_rows(scaled_error, groups.shards, 10)
    dec_bias_grad = jnp.sum(error_all, axis=0, dtype=jnp.float32)
    latent_part = lax.dot_general(
        error_all, dec_weight, (((1,), (1,)), ((), ())), preferred_element_type=jnp.float32
    )
    dec_grad = lax.dot_general(
        latents, error_all, (((0,), (0,)), ((), ())), preferred_element_type=jnp.float32
    )
    latent_grad = scatter_sum(latent_part.astype(jnp.bfloat16), groups.low, 11).astype(jnp.bfloat16)
    latent_grad = scatter_sum(latent_grad, groups.high, 12)
    my_grad = (latent_grad * jax.nn.sigmoid(4.0 * preact)).astype(jnp.bfloat16)
    preact_grad = gather_rows(gather_rows(my_grad, groups.high, 13), groups.low, 14)
    enc_grad = lax.dot_general(
        block, preact_grad, (((0,), (0,)), ((), ())), preferred_element_type=jnp.float32
    ).astype(jnp.bfloat16)
    enc_bias_grad = jnp.sum(preact_grad, axis=0, dtype=jnp.float32)
    return (layer_out, enc_grad, enc_bias_grad, dec_grad.astype(jnp.bfloat16), dec_bias_grad)


def solution(mesh):
    placed = (
        P(None, "wid", None),
        P(None, ("grp", "ctx"), "wid", None),
        P(None, ("grp", "ctx"), "wid", None),
        P(),
        P(),
        P("wid", ("grp", "ctx")),
        P("wid", ("grp", "ctx")),
        P("wid", ("grp", "ctx")),
        P(("grp", "ctx")),
        P(("grp", "ctx"), "wid"),
        P("wid"),
    )
    return jax.shard_map(
        functools.partial(body, dict(mesh.shape)),
        mesh=mesh,
        in_specs=placed,
        out_specs=(
            P("wid", ("grp", "ctx")),
            P("wid", ("grp", "ctx")),
            P(("grp", "ctx")),
            P(("grp", "ctx"), "wid"),
            P("wid"),
        ),
        check_vma=False,
    )
```

```python
import functools

import jax
import jax.numpy as jnp
from jax import lax
from jax.experimental import pallas as pl
from jax.experimental.pallas import tpu as pltpu
from jax.sharding import PartitionSpec as P

HD = 128
MESH = pl.DeviceIdType.MESH


def exchange_kernel(n, where, peer_id, gather, x_ref, out_ref, send_sem, recv_sem):
    me = where()
    peers = [lax.rem(me + step, n) for step in range(1, n)]
    barrier = pltpu.get_barrier_semaphore()
    for peer in peers:
        pl.semaphore_signal(barrier, inc=1, device_id=peer_id(peer), device_id_type=MESH)
    pl.semaphore_wait(barrier, n - 1)

    def copy_to(step, peer):
        return pltpu.make_async_remote_copy(
            src_ref=x_ref if gather else x_ref.at[peer],
            dst_ref=out_ref.at[me],
            send_sem=send_sem.at[step],
            recv_sem=recv_sem.at[me],
            device_id=peer_id(peer),
            device_id_type=MESH,
        )

    def copy_from(step, peer):
        return pltpu.make_async_remote_copy(
            src_ref=x_ref if gather else x_ref.at[peer],
            dst_ref=out_ref.at[peer],
            send_sem=send_sem.at[step],
            recv_sem=recv_sem.at[peer],
            device_id=peer_id(peer),
            device_id_type=MESH,
        )

    sends = [copy_to(step, peer) for step, peer in enumerate(peers)]
    for copy in sends:
        copy.start()
    out_ref[me] = x_ref[...] if gather else x_ref[me]
    for step, peer in enumerate(peers):
        copy_from(step, peer).wait_recv()
    for copy in sends:
        copy.wait_send()


def exchange(x, n, where, peer_id, gather, number):
    block = x.shape if gather else x.shape[1:]
    return pl.pallas_call(
        functools.partial(exchange_kernel, n, where, peer_id, gather),
        out_shape=jax.ShapeDtypeStruct((n,) + block, x.dtype),
        in_specs=[pl.BlockSpec(memory_space=pltpu.VMEM)],
        out_specs=pl.BlockSpec(memory_space=pltpu.VMEM),
        scratch_shapes=[pltpu.SemaphoreType.DMA((n,)), pltpu.SemaphoreType.DMA((n,))],
        compiler_params=pltpu.CompilerParams(
            collective_id=number, has_side_effects=True, vmem_limit_bytes=24 * 1024 * 1024
        ),
        name="exchange%d" % number,
    )(x)


class Groups:
    def __init__(self, sizes):
        ctx_n = sizes["ctx"]
        self.shards = (
            sizes["grp"] * ctx_n,
            lambda: lax.axis_index("grp") * ctx_n + lax.axis_index("ctx"),
            lambda p: {"grp": p // ctx_n, "ctx": lax.rem(p, ctx_n)},
        )
        self.wid = (sizes["wid"], lambda: lax.axis_index("wid"), lambda p: {"wid": p})
        self.low = (
            2,
            lambda: lax.rem(lax.axis_index("wid"), 2),
            lambda p: {"wid": (lax.axis_index("wid") // 2) * 2 + p},
        )
        self.high = (
            sizes["wid"] // 2,
            lambda: lax.axis_index("wid") // 2,
            lambda p: {"wid": p * 2 + lax.rem(lax.axis_index("wid"), 2)},
        )


def scatter_sum(x, group, number):
    n = group[0]
    parts = exchange(x.reshape((n, x.shape[0] // n) + x.shape[1:]), *group, False, number)
    return jnp.sum(parts.astype(jnp.float32), axis=0)


def gather_rows(x, group, number):
    whole = exchange(x, *group, True, number)
    return whole.reshape((whole.shape[0] * whole.shape[1],) + whole.shape[2:])


def rows_at(start, size):
    return pl.ds(pl.multiple_of(start, 16), size)


def cols_at(start, size):
    return pl.ds(pl.multiple_of(start, 128), size)


def partners(me, n):
    if n == 2:
        to = [1 - me]
        return to, to
    if n == 4:
        near = me + 1 - 2 * lax.rem(me, 2)
        to = [near, lax.rem(me + 2, 4), lax.rem(near + 2, 4)]
        return to, to
    return (
        [lax.rem(me + k, n) for k in range(1, n)],
        [lax.rem(me + n - k, n) for k in range(1, n)],
    )


class Plan:
    def __init__(self, sizes, query, keys, resid, enc_weight):
        self.grp, self.ctx, self.wid = sizes["grp"], sizes["ctx"], sizes["wid"]
        self.high = self.wid // 2
        self.shards = self.grp * self.ctx
        self.row_count, self.heads_local, self.head_dim = query.shape
        self.seqs, self.slots, self.kv_local = keys.shape[:3]
        self.heads = self.heads_local // self.kv_local
        self.width, self.latents = enc_weight.shape
        self.cols = resid.shape[1]
        self.streams = 2
        self.rows = self.row_count // self.streams
        self.half = self.rows // 2
        self.quarter = self.rows // self.wid
        self.side = self.rows // self.ctx
        self.piece = self.side // self.grp
        self.cuts = 5 if self.width % 640 == 0 else 2

    def fits(self):
        return (
            self.wid % 2 == 0
            and self.grp == self.wid == self.seqs
            and self.ctx == self.kv_local
            and self.ctx > 1
            and self.rows % (16 * self.wid) == 0
            and self.rows % (16 * self.shards) == 0
            and self.cols % 128 == 0
            and self.cols * self.ctx == self.width
            and self.width % (128 * self.cuts) == 0
            and self.latents % 512 == 0
            and self.head_dim % 128 == 0
            and self.heads % 2 == 0
        )


def fused_kernel(
    plan, query, cache, key_pos, position, resid, enc_bias, dec_bias, out_hbm, enc_hbm, dec_hbm,
    layer_out, block_t, lat_t, err, pgrad,
    out_w, enc_w, dec_w, kv, att, proj, opair_in, opair_sum, ohigh_in, zin, block, lat,
    part, pair_in, pair_sum, high_in, factor, recon, side_in, side_sum, piece_in,
    load_sem, kv_sem, att_sem, att_cross, opair_sem, ohigh_sem, lo_sem, blk_sem, blk_cross,
    pair_sem, high_sem, gather_sem, relay_sem, side_sem, piece_sem, spread_sem, cross_sem,
):
    p = plan
    g, c, w = lax.axis_index("grp"), lax.axis_index("ctx"), lax.axis_index("wid")
    low, high = lax.rem(w, 2), w // 2
    partner = {"wid": w + 1 - 2 * low}
    highs, highs_from = partners(high, p.high)
    ctxs, ctxs_from = partners(c, p.ctx)
    grps, grps_from = partners(g, p.grp)
    to_high = lambda h: {"wid": h * 2 + low}
    to_ctx = lambda q: {"ctx": q}
    to_grp = lambda q: {"grp": q}
    others = [(1 - low, high)] + [(low, h) for h in highs_from] + [(1 - low, h) for h in highs_from]
    shard_to = [(q, r) for q in [g] + grps for r in [c] + ctxs][1:]
    shard_from = [(q, r) for q in [g] + grps_from for r in [c] + ctxs_from][1:]

    enc_step = 512
    enc_steps = p.latents // enc_step

    def load(src, dst, index):
        copy = pltpu.make_async_copy(src, dst, load_sem.at[index])
        copy.start()
        return copy

    barrier = pltpu.get_barrier_semaphore()
    greeted = [{"grp": q, "ctx": r} for q, r in shard_to]
    greeted += [{"wid": hi * 2 + lo} for lo, hi in others]
    for peer in greeted:
        pl.semaphore_signal(barrier, inc=1, device_id=peer, device_id_type=MESH)
    out_load = load(out_hbm, out_w, 0)
    enc_load = load(enc_hbm, enc_w, 1)
    dec_load = load(dec_hbm, dec_w, 2)
    pl.semaphore_wait(barrier, len(greeted))

    pending = []

    def send(src, dst, sem, index, peer, to_index=None, when=None):
        copy = pltpu.make_async_remote_copy(
            src_ref=src, dst_ref=dst, send_sem=sem.at[(0,) + index],
            recv_sem=sem.at[(1,) + (index if to_index is None else to_index)],
            device_id=peer, device_id_type=MESH,
        )
        if when is None:
            copy.start()
        else:
            pl.when(when)(lambda: copy.start())
        pending.append((copy, when))

    def arrived(ref, sem, index):
        pltpu.make_async_remote_copy(
            src_ref=ref, dst_ref=ref, send_sem=sem.at[(0,) + index], recv_sem=sem.at[(1,) + index],
            device_id=partner, device_id_type=MESH,
        ).wait_recv()

    def quarter_row(t, lo, hi):
        return t * p.rows + (lo * p.high + hi) * p.quarter

    def piece_row(t, q, r):
        return t * p.rows + q * p.side + r * p.piece

    def shard(q, r):
        return q * p.ctx + r

    def loop(count, body):
        def step(i, carry):
            body(pl.multiple_of(i * 16, 16))
            return carry

        lax.fori_loop(0, count // 16, step, 0)

    def cache_send():
        for k, (q, r) in reversed(list(enumerate(shard_to))):
            send(
                cache.at[shard(q, r)], kv.at[rows_at(shard(g, c) * p.slots, p.slots)],
                kv_sem, (k,), {"grp": q, "ctx": r},
            )
        kv[rows_at(shard(g, c) * p.slots, p.slots)] = cache[shard(g, c)]

    def cache_wait():
        for k, (q, r) in enumerate(shard_from):
            arrived(kv.at[rows_at(shard(q, r) * p.slots, p.slots)], kv_sem, (k,))

    def att_at(t, q, r):
        return att.at[
            rows_at(quarter_row(t, lax.rem(q, 2), q // 2), p.quarter),
            cols_at(r * p.heads * p.head_dim, p.heads * p.head_dim),
        ]

    def attend_rows(t):
        two = 2 * p.quarter
        visible = key_pos[...] <= position[t]
        mine = att_at(t, g, c)
        for i in range(p.heads // 2):
            scores = lax.dot_general(
                query[t, pl.ds(i * two, two)], kv[:, : p.head_dim], (((1,), (1,)), ((), ())),
                preferred_element_type=jnp.float32,
            ) * p.head_dim ** (-0.5)
            peak = jnp.max(jnp.where(visible, scores, -1e30), axis=-1, keepdims=True)
            weights = jnp.where(visible, jnp.exp(scores - peak), 0.0)
            total = jnp.sum(weights, axis=-1, keepdims=True)
            weighted = jnp.dot(
                weights.astype(jnp.bfloat16), kv[:, p.head_dim :], preferred_element_type=jnp.float32
            )
            out = (weighted / total).astype(jnp.bfloat16)
            for j in range(2):
                mine[:, pl.ds((2 * i + j) * p.head_dim, p.head_dim)] = out[j * p.quarter : (j + 1) * p.quarter]
        for k, q in enumerate(grps):
            send(mine, mine, att_sem, (t, k), to_grp(q))
        for i, r in enumerate(ctxs):
            send(mine, mine, att_cross, (t, i, 0), to_ctx(r))

    def att_relay(t):
        for k, q in enumerate(grps_from):
            theirs = att_at(t, q, c)
            arrived(theirs, att_sem, (t, k))
            for i, r in enumerate(ctxs):
                send(theirs, theirs, att_cross, (t, i, k + 1), to_ctx(r))

    def project(t):
        for i, r in enumerate(ctxs_from):
            for k, q in enumerate([g] + grps_from):
                arrived(att_at(t, q, r), att_cross, (t, i, k))
        if t == 0:
            out_load.wait()
        rows = pl.ds(t * p.rows, p.rows)
        proj[rows] = jnp.dot(att[rows], out_w[...], preferred_element_type=jnp.float32).astype(jnp.bfloat16)
        send(
            proj.at[rows_at(t * p.rows + (1 - low) * p.half, p.half)], opair_in.at[t], opair_sem, (t,), partner
        )

    def project_add(t):
        arrived(opair_in.at[t], opair_sem, (t,))

        def body(r):
            mine = proj[rows_at(t * p.rows + low * p.half + r, 16)].astype(jnp.float32)
            opair_sum[t, pl.ds(r, 16)] = (mine + opair_in[t, pl.ds(r, 16)].astype(jnp.float32)).astype(jnp.bfloat16)

        loop(p.half, body)
        for s, h in enumerate(highs):
            send(opair_sum.at[t, rows_at(h * p.quarter, p.quarter)], ohigh_in.at[t, s], ohigh_sem, (t, s), to_high(h))

    def layer(t):
        for s in range(len(highs)):
            arrived(ohigh_in.at[t, s], ohigh_sem, (t, s))

        def body(r):
            total = opair_sum[t, rows_at(high * p.quarter + r, 16)].astype(jnp.float32)
            for s in range(len(highs)):
                total = total + ohigh_in[t, s, pl.ds(r, 16)].astype(jnp.float32)
            rows = rows_at(t * p.quarter + r, 16)
            value = (total + resid[rows].astype(jnp.float32)).astype(jnp.bfloat16)
            layer_out[rows] = value
            zin[t, g, pl.ds(r, 16)] = value

        loop(p.quarter, body)
        for k, q in enumerate(grps):
            send(zin.at[t, g], zin.at[t, g], lo_sem, (t, k), to_grp(q))

    def block_at(t, lo, hi, r):
        return block.at[rows_at(quarter_row(t, lo, hi), p.quarter), cols_at(r * p.cols, p.cols)]

    def block_relay(t):
        mine = block_at(t, low, high, c)
        for k, q in enumerate([g] + grps_from):
            if k:
                arrived(zin.at[t, q], lo_sem, (t, k - 1))
            owned, away = w == q, w != q

            @pl.when(owned)
            def _(q=q):
                mine[...] = zin[t, q]

            for i, r in enumerate(ctxs):
                send(mine, mine, blk_cross, (t, i, 0, k), to_ctx(r), (t, i, 0, 0), owned)
            send(zin.at[t, q], mine, blk_sem, (t, k), {"wid": q}, (t, w), away)

    def block_spread(t):
        for j, (lo, hi) in enumerate(others):
            theirs = block_at(t, lo, hi, c)
            arrived(theirs, blk_sem, (t, hi * 2 + lo))
            for i, r in enumerate(ctxs):
                send(theirs, theirs, blk_cross, (t, i, j + 1, 0), to_ctx(r))

    def block_wait(t):
        for i, r in enumerate(ctxs_from):
            for j, (lo, hi) in enumerate([(low, high)] + others):
                arrived(block_at(t, lo, hi, r), blk_cross, (t, i, j, 0))

    def pair_send(k, t):
        there = part.at[k, rows_at(t * p.rows + (1 - low) * p.half, p.half)]
        send(there, pair_in.at[k, t], pair_sem, (k, t), partner)

    def pair_add(k, t):
        arrived(pair_in.at[k, t], pair_sem, (k, t))

        def body(r):
            mine = part[k, rows_at(t * p.rows + low * p.half + r, 16)].astype(jnp.float32)
            pair_sum[k, t, pl.ds(r, 16)] = (mine + pair_in[k, t, pl.ds(r, 16)].astype(jnp.float32)).astype(jnp.bfloat16)

        loop(p.half, body)
        for s, h in enumerate(highs):
            send(pair_sum.at[k, t, rows_at(h * p.quarter, p.quarter)], high_in.at[k, t, s], high_sem, (k, t, s), to_high(h))

    def high_sum(k, t, r):
        total = pair_sum[k, t, rows_at(high * p.quarter + r, 16)].astype(jnp.float32)
        for s in range(len(highs)):
            total = total + high_in[k, t, s, pl.ds(r, 16)].astype(jnp.float32)
        return total

    def publish(k, t, out):
        mine = out.at[rows_at(quarter_row(t, low, high), p.quarter)]
        for s, h in enumerate(highs):
            send(mine, mine, gather_sem, (k, t, s + 1), to_high(h))
        send(mine, mine, gather_sem, (k, t, 0), partner)

    def activate(t):
        for s in range(len(highs)):
            arrived(high_in.at[0, t, s], high_sem, (0, t, s))

        def body(r):
            z = 4.0 * (high_sum(0, t, r) + enc_bias[...])
            e = jnp.exp(-jnp.abs(z))
            lat[rows_at(quarter_row(t, low, high) + r, 16)] = (
                (jnp.maximum(z, 0.0) + jnp.log1p(e)) * 0.25
            ).astype(jnp.bfloat16)
            factor[t, pl.ds(r, 16)] = jnp.where(z >= 0.0, 1.0, e) / (1.0 + e)

        loop(p.quarter, body)
        publish(0, t, lat)

    def cotangent(t):
        for s in range(len(highs)):
            arrived(high_in.at[1, t, s], high_sem, (1, t, s))

        def body(r):
            pgrad[rows_at(quarter_row(t, low, high) + r, 16)] = (
                high_sum(1, t, r) * factor[t, pl.ds(r, 16)]
            ).astype(jnp.bfloat16)

        loop(p.quarter, body)
        publish(1, t, pgrad)

    def relay(k, t, out):
        for s, h in enumerate(highs_from):
            theirs = out.at[rows_at(quarter_row(t, low, h), p.quarter)]
            arrived(theirs, gather_sem, (k, t, s + 1))
            send(theirs, theirs, relay_sem, (k, t, s), partner)

    def collected(k, t, out):
        arrived(out.at[rows_at(quarter_row(t, 1 - low, high), p.quarter)], gather_sem, (k, t, 0))
        for s, h in enumerate(highs_from):
            arrived(out.at[rows_at(quarter_row(t, 1 - low, h), p.quarter)], relay_sem, (k, t, s))

    def encode(t):
        block_wait(t)
        if t == 0:
            enc_load.wait()
        rows = pl.ds(t * p.rows, p.rows)

        def step(j, carry):
            cols = cols_at(j * enc_step, enc_step)
            part[0, rows, cols] = jnp.dot(
                block[rows, :], enc_w[:, cols], preferred_element_type=jnp.float32
            ).astype(jnp.bfloat16)
            return carry

        lax.fori_loop(0, enc_steps, step, 0)
        pair_send(0, t)

    cut = p.width // p.cuts

    def decode(t):
        collected(0, t, lat)
        if t == 0:
            dec_load.wait()
        rows = pl.ds(t * p.rows, p.rows)
        for j in range(p.cuts):
            cols = pl.ds(j * cut, cut)
            recon[rows, cols] = jnp.dot(
                lat[rows, :], dec_w[:, cols], preferred_element_type=jnp.float32
            ).astype(jnp.bfloat16)
            for s, q in enumerate(ctxs):
                send(
                    recon.at[rows_at(piece_row(t, q, 0), p.side), cols], side_in.at[t, s, :, cols],
                    side_sem, (t, j, s), to_ctx(q),
                )

    def side_add(t):
        for j in range(p.cuts):
            cols = pl.ds(j * cut, cut)
            for s in range(len(ctxs)):
                arrived(side_in.at[t, s, :, cols], side_sem, (t, j, s))
            total = recon[rows_at(piece_row(t, c, 0), p.side), cols].astype(jnp.float32)
            for s in range(len(ctxs)):
                total = total + side_in[t, s, :, cols].astype(jnp.float32)
            side_sum[t, :, cols] = total.astype(jnp.bfloat16)
            for s, q in enumerate(grps):
                send(
                    side_sum.at[t, rows_at(q * p.piece, p.piece), cols], piece_in.at[t, s, :, cols],
                    piece_sem, (t, j, s), to_grp(q),
                )

    def err_at(t, q, r, cols):
        return err.at[rows_at(piece_row(t, q, r), p.piece), cols]

    def error(t):
        for j in range(p.cuts):
            cols = pl.ds(j * cut, cut)
            for s in range(len(grps)):
                arrived(piece_in.at[t, s, :, cols], piece_sem, (t, j, s))
            total = side_sum[t, rows_at(g * p.piece, p.piece), cols].astype(jnp.float32)
            for s in range(len(grps)):
                total = total + piece_in[t, s, :, cols].astype(jnp.float32)
            rows = rows_at(piece_row(t, c, g), p.piece)
            wanted = block[rows, cols].astype(jnp.float32)
            err[rows, cols] = ((total + dec_bias[:, cols] - wanted) * p.row_count ** (-0.5)).astype(jnp.bfloat16)
            mine = err_at(t, c, g, cols)
            for s, q in enumerate(grps):
                send(mine, mine, spread_sem, (t, j, s), to_grp(q))
            for s, q in enumerate(ctxs):
                send(mine, mine, cross_sem, (t, j, s, 0), to_ctx(q))

    def error_relay(t):
        for j in range(p.cuts):
            cols = pl.ds(j * cut, cut)
            for i, r in enumerate(grps_from):
                theirs = err_at(t, c, r, cols)
                arrived(theirs, spread_sem, (t, j, i))
                for s, q in enumerate(ctxs):
                    send(theirs, theirs, cross_sem, (t, j, s, i + 1), to_ctx(q))

    def back(t):
        for j in range(p.cuts):
            for s, q in enumerate(ctxs_from):
                for i, r in enumerate([g] + grps_from):
                    arrived(err_at(t, q, r, pl.ds(j * cut, cut)), cross_sem, (t, j, s, i))
        rows = pl.ds(t * p.rows, p.rows)

        def step(j, carry):
            cols = pl.ds(pl.multiple_of(j * enc_step, enc_step), enc_step)
            part[1, rows, cols] = lax.dot_general(
                err[rows, :], dec_w[cols, :], (((1,), (1,)), ((), ())), preferred_element_type=jnp.float32
            ).astype(jnp.bfloat16)
            return carry

        lax.fori_loop(0, enc_steps, step, 0)
        pair_send(1, t)

    def turn(src, dst, t, count):
        rows = pl.ds(t * p.rows, p.rows)

        def step(j, carry):
            cols = cols_at(j * 256, 256)
            dst[cols, rows] = src[rows, cols].T
            return carry

        lax.fori_loop(0, count // 256, step, 0)

    cache_send()
    cache_wait()
    stages = [
        lambda: attend_rows(0),
        lambda: attend_rows(1),
        lambda: att_relay(0),
        lambda: att_relay(1),
        lambda: project(0),
        lambda: project(1),
        lambda: project_add(0),
        lambda: project_add(1),
        lambda: layer(0),
        lambda: layer(1),
        lambda: block_relay(0),
        lambda: block_spread(0),
        lambda: block_relay(1),
        lambda: block_spread(1),
        lambda: encode(0),
        lambda: encode(1),
        lambda: pair_add(0, 0),
        lambda: pair_add(0, 1),
        lambda: turn(block, block_t, 0, p.width),
        lambda: turn(block, block_t, 1, p.width),
        lambda: activate(0),
        lambda: activate(1),
        lambda: relay(0, 0, lat),
        lambda: decode(0),
        lambda: turn(lat, lat_t, 0, p.latents),
        lambda: relay(0, 1, lat),
        lambda: side_add(0),
        lambda: decode(1),
        lambda: error(0),
        lambda: side_add(1),
        lambda: turn(lat, lat_t, 1, p.latents),
        lambda: error_relay(0),
        lambda: error(1),
        lambda: back(0),
        lambda: error_relay(1),
        lambda: pair_add(1, 0),
        lambda: back(1),
        lambda: pair_add(1, 1),
        lambda: cotangent(0),
        lambda: cotangent(1),
        lambda: relay(1, 0, pgrad),
        lambda: relay(1, 1, pgrad),
        lambda: collected(1, 0, pgrad),
        lambda: collected(1, 1, pgrad),
    ]
    for stage in stages:
        stage()
    for copy, when in pending:
        if when is None:
            copy.wait_send()
        else:
            pl.when(when)(lambda copy=copy: copy.wait_send())


def fused(plan, query, keys, values, lengths, query_pos, resid, out_weight, enc_weight, enc_bias, dec_weight, dec_bias):
    p = plan
    low = jnp.bfloat16
    g, c = lax.axis_index("grp"), lax.axis_index("ctx")
    cache = jnp.concatenate([keys, values], axis=-1).transpose(0, 2, 1, 3)
    cache = cache.reshape(p.shards, p.slots, 2 * p.head_dim)
    seq_rows = p.row_count // p.seqs
    mine = lax.dynamic_slice(query, (g * seq_rows, c * p.heads, 0), (seq_rows, p.heads, p.head_dim))
    mine = mine.reshape(p.streams, p.quarter, p.heads, p.head_dim).transpose(0, 2, 1, 3)
    mine = mine.reshape(p.streams, p.heads * p.quarter, p.head_dim)
    live = lax.dynamic_index_in_dim(lengths, g, 0, keepdims=False)
    before = jnp.arange(p.shards)[None, :] < jnp.arange(p.shards)[:, None]
    offset = jnp.sum(jnp.where(before, live[None, :], 0), axis=1)
    slot_ids = jnp.arange(p.slots, dtype=jnp.int32)
    key_pos = jnp.where(
        slot_ids[None, :] < live[:, None], offset[:, None] + slot_ids[None, :], jnp.int32(2**30)
    ).reshape(1, -1)
    position = lax.dynamic_slice_in_dim(query_pos, g * seq_rows, seq_rows, 0).reshape(p.streams, 1, p.quarter)
    position = jnp.broadcast_to(position, (p.streams, 2, p.quarter)).reshape(p.streams, 2 * p.quarter, 1)

    vmem = pl.BlockSpec(memory_space=pltpu.VMEM)
    hbm = pl.BlockSpec(memory_space=pltpu.HBM)
    n, highs, ctxs, grps = p.streams, p.high - 1, p.ctx - 1, p.grp - 1
    dma = pltpu.SemaphoreType.DMA
    return pl.pallas_call(
        functools.partial(fused_kernel, p),
        out_shape=(
            jax.ShapeDtypeStruct((n * p.quarter, p.cols), low),
            jax.ShapeDtypeStruct((p.width, p.row_count), low),
            jax.ShapeDtypeStruct((p.latents, p.row_count), low),
            jax.ShapeDtypeStruct((p.row_count, p.width), low),
            jax.ShapeDtypeStruct((p.row_count, p.latents), low),
        ),
        in_specs=[vmem] * 7 + [hbm] * 3,
        out_specs=(vmem,) * 5,
        scratch_shapes=[
            pltpu.VMEM(out_weight.shape, low),
            pltpu.VMEM((p.width, p.latents), low),
            pltpu.VMEM((p.latents, p.width), low),
            pltpu.VMEM((p.shards * p.slots, 2 * p.head_dim), low),
            pltpu.VMEM((p.row_count, p.heads_local * p.head_dim), low),
            pltpu.VMEM((p.row_count, p.cols), low),
            pltpu.VMEM((n, p.half, p.cols), low),
            pltpu.VMEM((n, p.half, p.cols), low),
            pltpu.VMEM((n, highs, p.quarter, p.cols), low),
            pltpu.VMEM((n, p.grp, p.quarter, p.cols), low),
            pltpu.VMEM((p.row_count, p.width), low),
            pltpu.VMEM((p.row_count, p.latents), low),
            pltpu.VMEM((2, p.row_count, p.latents), low),
            pltpu.VMEM((2, n, p.half, p.latents), low),
            pltpu.VMEM((2, n, p.half, p.latents), low),
            pltpu.VMEM((2, n, highs, p.quarter, p.latents), low),
            pltpu.VMEM((n, p.quarter, p.latents), jnp.float32),
            pltpu.VMEM((p.row_count, p.width), low),
            pltpu.VMEM((n, ctxs, p.side, p.width), low),
            pltpu.VMEM((n, p.side, p.width), low),
            pltpu.VMEM((n, grps, p.piece, p.width), low),
            dma((3,)),
            dma((2, p.shards - 1)),
            dma((2, n, grps)),
            dma((2, n, ctxs, grps + 1)),
            dma((2, n)),
            dma((2, n, highs)),
            dma((2, n, grps)),
            dma((2, n, p.grp)),
            dma((2, n, ctxs, p.wid, p.grp)),
            dma((2, 2, n)),
            dma((2, 2, n, highs)),
            dma((2, 2, n, highs + 1)),
            dma((2, 2, n, highs)),
            dma((2, n, p.cuts, ctxs)),
            dma((2, n, p.cuts, grps)),
            dma((2, n, p.cuts, grps)),
            dma((2, n, p.cuts, ctxs, grps + 1)),
        ],
        compiler_params=pltpu.CompilerParams(
            collective_id=0, has_side_effects=True, vmem_limit_bytes=44 * 1024 * 1024
        ),
        name="fused",
    )(
        mine, cache, key_pos, position, resid, enc_bias.reshape(1, -1), dec_bias.reshape(1, -1),
        out_weight, enc_weight, dec_weight,
    )


def grads_kernel(dec_step, enc_step, depth, block_t, lat_t, err, pgrad, layer_in, enc_out, dec_out, enc_sum, dec_sum, layer_out, dec_buf, enc_buf, sem):
    layer_out[...] = layer_in[...]
    jobs = [(0, i) for i in range(dec_out.shape[0] // dec_step)]
    jobs += [(1, i) for i in range(enc_out.shape[0] // enc_step)]
    started = []
    for k, (kind, i) in enumerate(jobs):
        x, y, out, buf, step = ((lat_t, err, dec_out, dec_buf, dec_step), (block_t, pgrad, enc_out, enc_buf, enc_step))[kind]
        slot = i % depth
        if i >= depth:
            started[k - depth].wait()
        rows = pl.ds(i * step, step)
        buf[slot] = jnp.dot(x[rows, :], y[...], preferred_element_type=jnp.float32).astype(jnp.bfloat16)
        copy = pltpu.make_async_copy(buf.at[slot], out.at[rows], sem.at[kind, slot])
        copy.start()
        started.append(copy)
    dec_sum[...] = jnp.sum(err[...].astype(jnp.float32), axis=0, keepdims=True)
    enc_sum[...] = jnp.sum(pgrad[...].astype(jnp.float32), axis=0, keepdims=True)
    for k, (kind, i) in enumerate(jobs):
        count = sum(1 for job in jobs if job[0] == kind)
        if i >= count - depth:
            started[k].wait()


def grads(block_t, lat_t, err, pgrad, layer_in):
    width, latents = block_t.shape[0], lat_t.shape[0]
    vmem = pl.BlockSpec(memory_space=pltpu.VMEM)
    hbm = pl.BlockSpec(memory_space=pltpu.HBM)
    dec_step, enc_step, depth = 256, 128, 4
    enc, dec, enc_sum, dec_sum, layer_out = pl.pallas_call(
        functools.partial(grads_kernel, dec_step, enc_step, depth),
        out_shape=(
            jax.ShapeDtypeStruct((width, latents), jnp.bfloat16),
            jax.ShapeDtypeStruct((latents, width), jnp.bfloat16),
            jax.ShapeDtypeStruct((1, latents), jnp.float32),
            jax.ShapeDtypeStruct((1, width), jnp.float32),
            jax.ShapeDtypeStruct(layer_in.shape, layer_in.dtype),
        ),
        in_specs=[vmem] * 5,
        out_specs=(hbm, hbm, vmem, vmem, vmem),
        scratch_shapes=[
            pltpu.VMEM((depth, dec_step, width), jnp.bfloat16),
            pltpu.VMEM((depth, enc_step, latents), jnp.bfloat16),
            pltpu.SemaphoreType.DMA((2, depth)),
        ],
        compiler_params=pltpu.CompilerParams(vmem_limit_bytes=16 * 1024 * 1024),
        name="grads",
    )(block_t, lat_t, err, pgrad, layer_in)
    return layer_out, enc, enc_sum.reshape(-1), dec, dec_sum.reshape(-1)


def attend(groups, query, keys, values, lengths, query_pos):
    seq_count, slot_count, kv_local, head_dim = keys.shape
    row_count, heads_local = query.shape[:2]
    group_size = heads_local // kv_local
    shards = groups.shards[0]
    pairs = seq_count * kv_local
    chunks = shards // pairs
    rows = row_count // seq_count // chunks
    pair = lax.axis_index(("grp", "ctx")) // chunks
    seq, head = pair // kv_local, lax.rem(pair, kv_local)
    row0 = seq * (row_count // seq_count) + lax.rem(lax.axis_index(("grp", "ctx")), chunks) * rows
    cache = jnp.concatenate([keys, values], axis=-1).transpose(0, 2, 1, 3)
    cache = cache.reshape(pairs, slot_count, 2 * head_dim)
    if chunks > 1:
        cache = jnp.repeat(cache, chunks, axis=0)
    cache = exchange(cache, *groups.shards, False, 0).reshape(shards * slot_count, 2 * head_dim)
    q = lax.dynamic_slice(query, (row0, head * group_size, 0), (rows, group_size, head_dim))
    live = lax.dynamic_index_in_dim(lengths, seq, 0, keepdims=False)
    before = jnp.arange(shards)[None, :] < jnp.arange(shards)[:, None]
    offset = jnp.sum(jnp.where(before, live[None, :], 0), axis=1)
    slot_ids = jnp.arange(slot_count, dtype=jnp.int32)
    key_pos = jnp.where(
        slot_ids[None, :] < live[:, None], offset[:, None] + slot_ids[None, :], jnp.int32(2**30)
    ).reshape(-1)
    position = lax.dynamic_slice_in_dim(query_pos, row0, rows, 0)
    visible = (key_pos[None, :] <= position[:, None])[:, None, :]
    scores = jnp.einsum(
        "rgd,td->rgt", q, cache[:, :head_dim], preferred_element_type=jnp.float32
    ) * HD ** (-0.5)
    peak = jnp.max(jnp.where(visible, scores, -1e30), axis=-1, keepdims=True)
    weights = jnp.where(visible, jnp.exp(scores - peak), 0.0)
    weight_sum = jnp.sum(weights, axis=-1, keepdims=True)
    weighted = jnp.einsum(
        "rgt,td->rgd", weights.astype(jnp.bfloat16), cache[:, head_dim:],
        preferred_element_type=jnp.float32,
    )
    mine = (weighted / weight_sum).astype(jnp.bfloat16).reshape(rows, group_size * head_dim)
    attention = exchange(mine, *groups.shards, True, 1)
    attention = attention.reshape(seq_count, kv_local, chunks, rows, group_size * head_dim)
    return attention.transpose(0, 2, 3, 1, 4).reshape(row_count, heads_local * head_dim)


def body(
    sizes,
    query,
    keys,
    values,
    lengths,
    query_pos,
    resid,
    out_weight,
    enc_weight,
    enc_bias,
    dec_weight,
    dec_bias,
):
    plan = Plan(sizes, query, keys, resid, enc_weight)
    if plan.fits():
        layer_out, block_t, lat_t, err, pgrad = fused(
            plan, query, keys, values, lengths, query_pos, resid, out_weight,
            enc_weight, enc_bias, dec_weight, dec_bias,
        )
        return grads(block_t, lat_t, err, pgrad, layer_out)
    groups = Groups(sizes)
    row_count = query.shape[0]
    shard_pos = lax.axis_index(("grp", "ctx"))
    attention = attend(groups, query, keys, values, lengths, query_pos)
    projected = jnp.dot(attention, out_weight, preferred_element_type=jnp.float32)
    mixed = scatter_sum(projected.astype(jnp.bfloat16), groups.wid, 2)
    layer_out = (mixed + resid.astype(jnp.float32)).astype(jnp.bfloat16)
    rows, cols = layer_out.shape
    wid_n = sizes["wid"]
    wide = exchange(layer_out, *groups.shards, True, 3)
    wide = wide.reshape(wid_n, -1, rows, cols).transpose(0, 2, 1, 3).reshape(wid_n, rows, -1)
    block = exchange(wide, *groups.wid, False, 4).reshape(row_count, -1)
    enc_part = jnp.dot(block, enc_weight, preferred_element_type=jnp.float32)
    preact = scatter_sum(enc_part.astype(jnp.bfloat16), groups.low, 5).astype(jnp.bfloat16)
    preact = scatter_sum(preact, groups.high, 6) + enc_bias
    my_latents = (jax.nn.softplus(4.0 * preact) * 0.25).astype(jnp.bfloat16)
    latents = gather_rows(gather_rows(my_latents, groups.high, 7), groups.low, 8)
    row_scale = row_count ** (-0.5)
    recon = jnp.dot(latents, dec_weight, preferred_element_type=jnp.float32)
    recon = scatter_sum(recon.astype(jnp.bfloat16), groups.shards, 9)
    piece_len = recon.shape[0]
    target = lax.dynamic_slice_in_dim(block, shard_pos * piece_len, piece_len, 0).astype(
        jnp.float32
    )
    scaled_error = ((recon + dec_bias - target) * row_scale).astype(jnp.bfloat16)
    error_all = gather_rows(scaled_error, groups.shards, 10)
    dec_bias_grad = jnp.sum(error_all, axis=0, dtype=jnp.float32)
    latent_part = lax.dot_general(
        error_all, dec_weight, (((1,), (1,)), ((), ())), preferred_element_type=jnp.float32
    )
    dec_grad = lax.dot_general(
        latents, error_all, (((0,), (0,)), ((), ())), preferred_element_type=jnp.float32
    )
    latent_grad = scatter_sum(latent_part.astype(jnp.bfloat16), groups.low, 11).astype(jnp.bfloat16)
    latent_grad = scatter_sum(latent_grad, groups.high, 12)
    my_grad = (latent_grad * jax.nn.sigmoid(4.0 * preact)).astype(jnp.bfloat16)
    preact_grad = gather_rows(gather_rows(my_grad, groups.high, 13), groups.low, 14)
    enc_grad = lax.dot_general(
        block, preact_grad, (((0,), (0,)), ((), ())), preferred_element_type=jnp.float32
    ).astype(jnp.bfloat16)
    enc_bias_grad = jnp.sum(preact_grad, axis=0, dtype=jnp.float32)
    return (layer_out, enc_grad, enc_bias_grad, dec_grad.astype(jnp.bfloat16), dec_bias_grad)


def solution(mesh):
    placed = (
        P(None, "wid", None),
        P(None, ("grp", "ctx"), "wid", None),
        P(None, ("grp", "ctx"), "wid", None),
        P(),
        P(),
        P("wid", ("grp", "ctx")),
        P("wid", ("grp", "ctx")),
        P("wid", ("grp", "ctx")),
        P(("grp", "ctx")),
        P(("grp", "ctx"), "wid"),
        P("wid"),
    )
    return jax.shard_map(
        functools.partial(body, dict(mesh.shape)),
        mesh=mesh,
        in_specs=placed,
        out_specs=(
            P("wid", ("grp", "ctx")),
            P("wid", ("grp", "ctx")),
            P(("grp", "ctx")),
            P(("grp", "ctx"), "wid"),
            P("wid"),
        ),
        check_vma=False,
    )
```

```python
import functools

import jax
import jax.numpy as jnp
from jax import lax
from jax.experimental import pallas as pl
from jax.experimental.pallas import tpu as pltpu
from jax.sharding import PartitionSpec as P

HD = 128
MESH = pl.DeviceIdType.MESH


def exchange_kernel(n, where, peer_id, gather, x_ref, out_ref, send_sem, recv_sem):
    me = where()
    peers = [lax.rem(me + step, n) for step in range(1, n)]
    barrier = pltpu.get_barrier_semaphore()
    for peer in peers:
        pl.semaphore_signal(barrier, inc=1, device_id=peer_id(peer), device_id_type=MESH)
    pl.semaphore_wait(barrier, n - 1)

    def copy_to(step, peer):
        return pltpu.make_async_remote_copy(
            src_ref=x_ref if gather else x_ref.at[peer],
            dst_ref=out_ref.at[me],
            send_sem=send_sem.at[step],
            recv_sem=recv_sem.at[me],
            device_id=peer_id(peer),
            device_id_type=MESH,
        )

    def copy_from(step, peer):
        return pltpu.make_async_remote_copy(
            src_ref=x_ref if gather else x_ref.at[peer],
            dst_ref=out_ref.at[peer],
            send_sem=send_sem.at[step],
            recv_sem=recv_sem.at[peer],
            device_id=peer_id(peer),
            device_id_type=MESH,
        )

    sends = [copy_to(step, peer) for step, peer in enumerate(peers)]
    for copy in sends:
        copy.start()
    out_ref[me] = x_ref[...] if gather else x_ref[me]
    for step, peer in enumerate(peers):
        copy_from(step, peer).wait_recv()
    for copy in sends:
        copy.wait_send()


def exchange(x, n, where, peer_id, gather, number):
    block = x.shape if gather else x.shape[1:]
    return pl.pallas_call(
        functools.partial(exchange_kernel, n, where, peer_id, gather),
        out_shape=jax.ShapeDtypeStruct((n,) + block, x.dtype),
        in_specs=[pl.BlockSpec(memory_space=pltpu.VMEM)],
        out_specs=pl.BlockSpec(memory_space=pltpu.VMEM),
        scratch_shapes=[pltpu.SemaphoreType.DMA((n,)), pltpu.SemaphoreType.DMA((n,))],
        compiler_params=pltpu.CompilerParams(
            collective_id=number, has_side_effects=True, vmem_limit_bytes=24 * 1024 * 1024
        ),
        name="exchange%d" % number,
    )(x)


class Groups:
    def __init__(self, sizes):
        ctx_n = sizes["ctx"]
        self.shards = (
            sizes["grp"] * ctx_n,
            lambda: lax.axis_index("grp") * ctx_n + lax.axis_index("ctx"),
            lambda p: {"grp": p // ctx_n, "ctx": lax.rem(p, ctx_n)},
        )
        self.wid = (sizes["wid"], lambda: lax.axis_index("wid"), lambda p: {"wid": p})
        self.low = (
            2,
            lambda: lax.rem(lax.axis_index("wid"), 2),
            lambda p: {"wid": (lax.axis_index("wid") // 2) * 2 + p},
        )
        self.high = (
            sizes["wid"] // 2,
            lambda: lax.axis_index("wid") // 2,
            lambda p: {"wid": p * 2 + lax.rem(lax.axis_index("wid"), 2)},
        )


def scatter_sum(x, group, number):
    n = group[0]
    parts = exchange(x.reshape((n, x.shape[0] // n) + x.shape[1:]), *group, False, number)
    return jnp.sum(parts.astype(jnp.float32), axis=0)


def gather_rows(x, group, number):
    whole = exchange(x, *group, True, number)
    return whole.reshape((whole.shape[0] * whole.shape[1],) + whole.shape[2:])


def rows_at(start, size):
    return pl.ds(pl.multiple_of(start, 16), size)


def cols_at(start, size):
    return pl.ds(pl.multiple_of(start, 128), size)


def partners(me, n):
    if n == 2:
        to = [1 - me]
        return to, to
    if n == 4:
        near = me + 1 - 2 * lax.rem(me, 2)
        to = [near, lax.rem(me + 2, 4), lax.rem(near + 2, 4)]
        return to, to
    return (
        [lax.rem(me + k, n) for k in range(1, n)],
        [lax.rem(me + n - k, n) for k in range(1, n)],
    )


class Plan:
    def __init__(self, sizes, query, keys, resid, enc_weight):
        self.grp, self.ctx, self.wid = sizes["grp"], sizes["ctx"], sizes["wid"]
        self.high = self.wid // 2
        self.shards = self.grp * self.ctx
        self.row_count, self.heads_local, self.head_dim = query.shape
        self.seqs, self.slots, self.kv_local = keys.shape[:3]
        self.heads = self.heads_local // self.kv_local
        self.width, self.latents = enc_weight.shape
        self.cols = resid.shape[1]
        self.streams = 2
        self.rows = self.row_count // self.streams
        self.half = self.rows // 2
        self.quarter = self.rows // self.wid
        self.side = self.rows // self.ctx
        self.piece = self.side // self.grp
        self.cuts = 5 if self.width % 640 == 0 else 2

    def fits(self):
        return (
            self.wid % 2 == 0
            and self.grp == self.wid == self.seqs
            and self.ctx == self.kv_local
            and self.ctx > 1
            and self.rows % (16 * self.wid) == 0
            and self.rows % (16 * self.shards) == 0
            and self.cols % 128 == 0
            and self.cols * self.ctx == self.width
            and self.width % (128 * self.cuts) == 0
            and self.latents % 512 == 0
            and self.head_dim % 128 == 0
            and self.heads % 2 == 0
        )


def fused_kernel(
    plan, query, cache, len_hbm, pos_hbm, resid_hbm, eb_hbm, db_hbm, out_hbm, enc_hbm, dec_hbm,
    layer_out, block_t, lat_t, err, pgrad,
    lengths, query_pos, resid, enc_bias, dec_bias, out_w, enc_w, dec_w, kv, att, proj, opair_in, opair_sum, ohigh_in, zin, block, lat,
    part, pair_in, pair_sum, high_in, factor, recon, side_in, side_sum, piece_in,
    load_sem, kv_sem, att_sem, att_cross, opair_sem, ohigh_sem, lo_sem, blk_sem, blk_cross,
    pair_sem, high_sem, gather_sem, relay_sem, side_sem, piece_sem, spread_sem, cross_sem,
):
    p = plan
    g, c, w = lax.axis_index("grp"), lax.axis_index("ctx"), lax.axis_index("wid")
    low, high = lax.rem(w, 2), w // 2
    partner = {"wid": w + 1 - 2 * low}
    highs, highs_from = partners(high, p.high)
    ctxs, ctxs_from = partners(c, p.ctx)
    grps, grps_from = partners(g, p.grp)
    to_high = lambda h: {"wid": h * 2 + low}
    to_ctx = lambda q: {"ctx": q}
    to_grp = lambda q: {"grp": q}
    others = [(1 - low, high)] + [(low, h) for h in highs_from] + [(1 - low, h) for h in highs_from]
    shard_to = [(q, r) for q in [g] + grps for r in [c] + ctxs][1:]
    shard_from = [(q, r) for q in [g] + grps_from for r in [c] + ctxs_from][1:]

    enc_step = 512
    enc_steps = p.latents // enc_step

    def load(src, dst, index):
        copy = pltpu.make_async_copy(src, dst, load_sem.at[index])
        copy.start()
        return copy

    barrier = pltpu.get_barrier_semaphore()
    greeted = [{"grp": q, "ctx": r} for q, r in shard_to]
    greeted += [{"wid": hi * 2 + lo} for lo, hi in others]
    for peer in greeted:
        pl.semaphore_signal(barrier, inc=1, device_id=peer, device_id_type=MESH)
    small_loads = [
        load(src, dst, 3 + k)
        for k, (src, dst) in enumerate(
            [(len_hbm, lengths), (pos_hbm, query_pos), (resid_hbm, resid), (eb_hbm, enc_bias), (db_hbm, dec_bias)]
        )
    ]
    out_load = load(out_hbm, out_w, 0)
    enc_load = load(enc_hbm, enc_w, 1)
    dec_load = load(dec_hbm, dec_w, 2)
    pl.semaphore_wait(barrier, len(greeted))

    pending = []

    def send(src, dst, sem, index, peer, to_index=None, when=None):
        copy = pltpu.make_async_remote_copy(
            src_ref=src, dst_ref=dst, send_sem=sem.at[(0,) + index],
            recv_sem=sem.at[(1,) + (index if to_index is None else to_index)],
            device_id=peer, device_id_type=MESH,
        )
        if when is None:
            copy.start()
        else:
            pl.when(when)(lambda: copy.start())
        pending.append((copy, when))

    def arrived(ref, sem, index):
        pltpu.make_async_remote_copy(
            src_ref=ref, dst_ref=ref, send_sem=sem.at[(0,) + index], recv_sem=sem.at[(1,) + index],
            device_id=partner, device_id_type=MESH,
        ).wait_recv()

    def quarter_row(t, lo, hi):
        return t * p.rows + (lo * p.high + hi) * p.quarter

    def piece_row(t, q, r):
        return t * p.rows + q * p.side + r * p.piece

    def shard(q, r):
        return q * p.ctx + r

    def loop(count, body):
        def step(i, carry):
            body(pl.multiple_of(i * 16, 16))
            return carry

        lax.fori_loop(0, count // 16, step, 0)

    def cache_send():
        for k, (q, r) in reversed(list(enumerate(shard_to))):
            send(
                cache.at[shard(q, r)], kv.at[rows_at(shard(g, c) * p.slots, p.slots)],
                kv_sem, (k,), {"grp": q, "ctx": r},
            )
        kv[rows_at(shard(g, c) * p.slots, p.slots)] = cache[shard(g, c)]

    def cache_wait():
        for k, (q, r) in enumerate(shard_from):
            arrived(kv.at[rows_at(shard(q, r) * p.slots, p.slots)], kv_sem, (k,))

    def att_at(t, q, r):
        return att.at[
            rows_at(quarter_row(t, lax.rem(q, 2), q // 2), p.quarter),
            cols_at(r * p.heads * p.head_dim, p.heads * p.head_dim),
        ]

    def key_positions():
        live = lengths[pl.ds(g, 1), :]
        slot = lax.broadcasted_iota(jnp.int32, (1, p.shards * p.slots), 1)
        key = jnp.full((1, p.shards * p.slots), 2**30, jnp.int32)
        offset = jnp.zeros((1, 1), jnp.int32)
        for b in range(p.shards):
            count = live[:, b : b + 1]
            own = slot - b * p.slots
            key = jnp.where((own >= 0) & (own < p.slots) & (own < count), offset + own, key)
            offset = offset + count
        return key

    def row_positions(t):
        shape = (2 * p.quarter, p.row_count)
        row = lax.broadcasted_iota(jnp.int32, shape, 0)
        wanted = lax.rem(row, p.quarter) + (g * (p.row_count // p.seqs) + t * p.quarter)
        here = lax.broadcasted_iota(jnp.int32, shape, 1) == wanted
        values = jnp.where(here, query_pos[...].reshape(1, -1).astype(jnp.float32), 0.0)
        return jnp.sum(values, axis=1, keepdims=True).astype(jnp.int32)

    def attend_rows(t):
        two = 2 * p.quarter
        visible = key_positions() <= row_positions(t)
        mine = att_at(t, g, c)
        for i in range(p.heads // 2):
            scores = lax.dot_general(
                query[t, pl.ds(i * two, two)], kv[:, : p.head_dim], (((1,), (1,)), ((), ())),
                preferred_element_type=jnp.float32,
            ) * p.head_dim ** (-0.5)
            peak = jnp.max(jnp.where(visible, scores, -1e30), axis=-1, keepdims=True)
            weights = jnp.where(visible, jnp.exp(scores - peak), 0.0)
            total = jnp.sum(weights, axis=-1, keepdims=True)
            weighted = jnp.dot(
                weights.astype(jnp.bfloat16), kv[:, p.head_dim :], preferred_element_type=jnp.float32
            )
            out = (weighted / total).astype(jnp.bfloat16)
            for j in range(2):
                mine[:, pl.ds((2 * i + j) * p.head_dim, p.head_dim)] = out[j * p.quarter : (j + 1) * p.quarter]
        for k, q in enumerate(grps):
            send(mine, mine, att_sem, (t, k), to_grp(q))
        for i, r in enumerate(ctxs):
            send(mine, mine, att_cross, (t, i, 0), to_ctx(r))

    def att_relay(t):
        for k, q in enumerate(grps_from):
            theirs = att_at(t, q, c)
            arrived(theirs, att_sem, (t, k))
            for i, r in enumerate(ctxs):
                send(theirs, theirs, att_cross, (t, i, k + 1), to_ctx(r))

    def project(t):
        for i, r in enumerate(ctxs_from):
            for k, q in enumerate([g] + grps_from):
                arrived(att_at(t, q, r), att_cross, (t, i, k))
        if t == 0:
            out_load.wait()
        rows = pl.ds(t * p.rows, p.rows)
        proj[rows] = jnp.dot(att[rows], out_w[...], preferred_element_type=jnp.float32).astype(jnp.bfloat16)
        send(
            proj.at[rows_at(t * p.rows + (1 - low) * p.half, p.half)], opair_in.at[t], opair_sem, (t,), partner
        )

    def project_add(t):
        arrived(opair_in.at[t], opair_sem, (t,))

        def body(r):
            mine = proj[rows_at(t * p.rows + low * p.half + r, 16)].astype(jnp.float32)
            opair_sum[t, pl.ds(r, 16)] = (mine + opair_in[t, pl.ds(r, 16)].astype(jnp.float32)).astype(jnp.bfloat16)

        loop(p.half, body)
        for s, h in enumerate(highs):
            send(opair_sum.at[t, rows_at(h * p.quarter, p.quarter)], ohigh_in.at[t, s], ohigh_sem, (t, s), to_high(h))

    def layer(t):
        for s in range(len(highs)):
            arrived(ohigh_in.at[t, s], ohigh_sem, (t, s))

        def body(r):
            total = opair_sum[t, rows_at(high * p.quarter + r, 16)].astype(jnp.float32)
            for s in range(len(highs)):
                total = total + ohigh_in[t, s, pl.ds(r, 16)].astype(jnp.float32)
            rows = rows_at(t * p.quarter + r, 16)
            value = (total + resid[rows].astype(jnp.float32)).astype(jnp.bfloat16)
            layer_out[rows] = value
            zin[t, g, pl.ds(r, 16)] = value

        loop(p.quarter, body)
        for k, q in enumerate(grps):
            send(zin.at[t, g], zin.at[t, g], lo_sem, (t, k), to_grp(q))

    def block_at(t, lo, hi, r):
        return block.at[rows_at(quarter_row(t, lo, hi), p.quarter), cols_at(r * p.cols, p.cols)]

    def block_relay(t):
        mine = block_at(t, low, high, c)
        for k, q in enumerate([g] + grps_from):
            if k:
                arrived(zin.at[t, q], lo_sem, (t, k - 1))
            owned, away = w == q, w != q

            @pl.when(owned)
            def _(q=q):
                mine[...] = zin[t, q]

            for i, r in enumerate(ctxs):
                send(mine, mine, blk_cross, (t, i, 0, k), to_ctx(r), (t, i, 0, 0), owned)
            send(zin.at[t, q], mine, blk_sem, (t, k), {"wid": q}, (t, w), away)

    def block_spread(t):
        for j, (lo, hi) in enumerate(others):
            theirs = block_at(t, lo, hi, c)
            arrived(theirs, blk_sem, (t, hi * 2 + lo))
            for i, r in enumerate(ctxs):
                send(theirs, theirs, blk_cross, (t, i, j + 1, 0), to_ctx(r))

    def block_wait(t):
        for i, r in enumerate(ctxs_from):
            for j, (lo, hi) in enumerate([(low, high)] + others):
                arrived(block_at(t, lo, hi, r), blk_cross, (t, i, j, 0))

    def pair_send(k, t):
        there = part.at[k, rows_at(t * p.rows + (1 - low) * p.half, p.half)]
        send(there, pair_in.at[k, t], pair_sem, (k, t), partner)

    def pair_add(k, t):
        arrived(pair_in.at[k, t], pair_sem, (k, t))

        def body(r):
            mine = part[k, rows_at(t * p.rows + low * p.half + r, 16)].astype(jnp.float32)
            pair_sum[k, t, pl.ds(r, 16)] = (mine + pair_in[k, t, pl.ds(r, 16)].astype(jnp.float32)).astype(jnp.bfloat16)

        loop(p.half, body)
        for s, h in enumerate(highs):
            send(pair_sum.at[k, t, rows_at(h * p.quarter, p.quarter)], high_in.at[k, t, s], high_sem, (k, t, s), to_high(h))

    def high_sum(k, t, r):
        total = pair_sum[k, t, rows_at(high * p.quarter + r, 16)].astype(jnp.float32)
        for s in range(len(highs)):
            total = total + high_in[k, t, s, pl.ds(r, 16)].astype(jnp.float32)
        return total

    def publish(k, t, out):
        mine = out.at[rows_at(quarter_row(t, low, high), p.quarter)]
        for s, h in enumerate(highs):
            send(mine, mine, gather_sem, (k, t, s + 1), to_high(h))
        send(mine, mine, gather_sem, (k, t, 0), partner)

    def activate(t):
        for s in range(len(highs)):
            arrived(high_in.at[0, t, s], high_sem, (0, t, s))

        def body(r):
            z = 4.0 * (high_sum(0, t, r) + enc_bias[...].reshape(1, -1))
            e = jnp.exp(-jnp.abs(z))
            lat[rows_at(quarter_row(t, low, high) + r, 16)] = (
                (jnp.maximum(z, 0.0) + jnp.log1p(e)) * 0.25
            ).astype(jnp.bfloat16)
            factor[t, pl.ds(r, 16)] = jnp.where(z >= 0.0, 1.0, e) / (1.0 + e)

        loop(p.quarter, body)
        publish(0, t, lat)

    def cotangent(t):
        for s in range(len(highs)):
            arrived(high_in.at[1, t, s], high_sem, (1, t, s))

        def body(r):
            pgrad[rows_at(quarter_row(t, low, high) + r, 16)] = (
                high_sum(1, t, r) * factor[t, pl.ds(r, 16)]
            ).astype(jnp.bfloat16)

        loop(p.quarter, body)
        publish(1, t, pgrad)

    def relay(k, t, out):
        for s, h in enumerate(highs_from):
            theirs = out.at[rows_at(quarter_row(t, low, h), p.quarter)]
            arrived(theirs, gather_sem, (k, t, s + 1))
            send(theirs, theirs, relay_sem, (k, t, s), partner)

    def collected(k, t, out):
        arrived(out.at[rows_at(quarter_row(t, 1 - low, high), p.quarter)], gather_sem, (k, t, 0))
        for s, h in enumerate(highs_from):
            arrived(out.at[rows_at(quarter_row(t, 1 - low, h), p.quarter)], relay_sem, (k, t, s))

    def encode(t):
        block_wait(t)
        if t == 0:
            enc_load.wait()
        rows = pl.ds(t * p.rows, p.rows)

        def step(j, carry):
            cols = cols_at(j * enc_step, enc_step)
            part[0, rows, cols] = jnp.dot(
                block[rows, :], enc_w[:, cols], preferred_element_type=jnp.float32
            ).astype(jnp.bfloat16)
            return carry

        lax.fori_loop(0, enc_steps, step, 0)
        pair_send(0, t)

    cut = p.width // p.cuts

    def decode(t):
        collected(0, t, lat)
        if t == 0:
            dec_load.wait()
        rows = pl.ds(t * p.rows, p.rows)
        for j in range(p.cuts):
            cols = pl.ds(j * cut, cut)
            recon[rows, cols] = jnp.dot(
                lat[rows, :], dec_w[:, cols], preferred_element_type=jnp.float32
            ).astype(jnp.bfloat16)
            for s, q in enumerate(ctxs):
                send(
                    recon.at[rows_at(piece_row(t, q, 0), p.side), cols], side_in.at[t, s, :, cols],
                    side_sem, (t, j, s), to_ctx(q),
                )

    def side_add(t):
        for j in range(p.cuts):
            cols = pl.ds(j * cut, cut)
            for s in range(len(ctxs)):
                arrived(side_in.at[t, s, :, cols], side_sem, (t, j, s))
            total = recon[rows_at(piece_row(t, c, 0), p.side), cols].astype(jnp.float32)
            for s in range(len(ctxs)):
                total = total + side_in[t, s, :, cols].astype(jnp.float32)
            side_sum[t, :, cols] = total.astype(jnp.bfloat16)
            for s, q in enumerate(grps):
                send(
                    side_sum.at[t, rows_at(q * p.piece, p.piece), cols], piece_in.at[t, s, :, cols],
                    piece_sem, (t, j, s), to_grp(q),
                )

    def err_at(t, q, r, cols):
        return err.at[rows_at(piece_row(t, q, r), p.piece), cols]

    def error(t):
        for j in range(p.cuts):
            cols = pl.ds(j * cut, cut)
            for s in range(len(grps)):
                arrived(piece_in.at[t, s, :, cols], piece_sem, (t, j, s))
            total = side_sum[t, rows_at(g * p.piece, p.piece), cols].astype(jnp.float32)
            for s in range(len(grps)):
                total = total + piece_in[t, s, :, cols].astype(jnp.float32)
            rows = rows_at(piece_row(t, c, g), p.piece)
            wanted = block[rows, cols].astype(jnp.float32)
            err[rows, cols] = ((total + dec_bias[cols].reshape(1, -1) - wanted) * p.row_count ** (-0.5)).astype(jnp.bfloat16)
            mine = err_at(t, c, g, cols)
            for s, q in enumerate(grps):
                send(mine, mine, spread_sem, (t, j, s), to_grp(q))
            for s, q in enumerate(ctxs):
                send(mine, mine, cross_sem, (t, j, s, 0), to_ctx(q))

    def error_relay(t):
        for j in range(p.cuts):
            cols = pl.ds(j * cut, cut)
            for i, r in enumerate(grps_from):
                theirs = err_at(t, c, r, cols)
                arrived(theirs, spread_sem, (t, j, i))
                for s, q in enumerate(ctxs):
                    send(theirs, theirs, cross_sem, (t, j, s, i + 1), to_ctx(q))

    def back(t):
        for j in range(p.cuts):
            for s, q in enumerate(ctxs_from):
                for i, r in enumerate([g] + grps_from):
                    arrived(err_at(t, q, r, pl.ds(j * cut, cut)), cross_sem, (t, j, s, i))
        rows = pl.ds(t * p.rows, p.rows)

        def step(j, carry):
            cols = pl.ds(pl.multiple_of(j * enc_step, enc_step), enc_step)
            part[1, rows, cols] = lax.dot_general(
                err[rows, :], dec_w[cols, :], (((1,), (1,)), ((), ())), preferred_element_type=jnp.float32
            ).astype(jnp.bfloat16)
            return carry

        lax.fori_loop(0, enc_steps, step, 0)
        pair_send(1, t)

    def turn(src, dst, t, count):
        rows = pl.ds(t * p.rows, p.rows)

        def step(j, carry):
            cols = cols_at(j * 256, 256)
            dst[cols, rows] = src[rows, cols].T
            return carry

        lax.fori_loop(0, count // 256, step, 0)

    cache_send()
    for copy in small_loads:
        copy.wait()
    cache_wait()
    stages = [
        lambda: attend_rows(0),
        lambda: attend_rows(1),
        lambda: att_relay(0),
        lambda: project(0),
        lambda: att_relay(1),
        lambda: project_add(0),
        lambda: project(1),
        lambda: layer(0),
        lambda: project_add(1),
        lambda: block_relay(0),
        lambda: layer(1),
        lambda: block_spread(0),
        lambda: block_relay(1),
        lambda: block_spread(1),
        lambda: encode(0),
        lambda: pair_add(0, 0),
        lambda: encode(1),
        lambda: pair_add(0, 1),
        lambda: turn(block, block_t, 0, p.width),
        lambda: turn(block, block_t, 1, p.width),
        lambda: activate(0),
        lambda: activate(1),
        lambda: relay(0, 0, lat),
        lambda: decode(0),
        lambda: turn(lat, lat_t, 0, p.latents),
        lambda: relay(0, 1, lat),
        lambda: side_add(0),
        lambda: decode(1),
        lambda: error(0),
        lambda: side_add(1),
        lambda: turn(lat, lat_t, 1, p.latents),
        lambda: error_relay(0),
        lambda: error(1),
        lambda: back(0),
        lambda: error_relay(1),
        lambda: pair_add(1, 0),
        lambda: back(1),
        lambda: pair_add(1, 1),
        lambda: cotangent(0),
        lambda: cotangent(1),
        lambda: relay(1, 0, pgrad),
        lambda: relay(1, 1, pgrad),
        lambda: collected(1, 0, pgrad),
        lambda: collected(1, 1, pgrad),
    ]
    for stage in stages:
        stage()
    for copy, when in pending:
        if when is None:
            copy.wait_send()
        else:
            pl.when(when)(lambda copy=copy: copy.wait_send())


def fused(plan, query, keys, values, lengths, query_pos, resid, out_weight, enc_weight, enc_bias, dec_weight, dec_bias):
    p = plan
    low = jnp.bfloat16
    g, c = lax.axis_index("grp"), lax.axis_index("ctx")
    cache = jnp.concatenate([keys, values], axis=-1).transpose(0, 2, 1, 3)
    cache = cache.reshape(p.shards, p.slots, 2 * p.head_dim)
    seq_rows = p.row_count // p.seqs
    mine = lax.dynamic_slice(query, (g * seq_rows, c * p.heads, 0), (seq_rows, p.heads, p.head_dim))
    mine = mine.reshape(p.streams, p.quarter, p.heads, p.head_dim).transpose(0, 2, 1, 3)
    mine = mine.reshape(p.streams, p.heads * p.quarter, p.head_dim)

    vmem = pl.BlockSpec(memory_space=pltpu.VMEM)
    hbm = pl.BlockSpec(memory_space=pltpu.HBM)
    n, highs, ctxs, grps = p.streams, p.high - 1, p.ctx - 1, p.grp - 1
    dma = pltpu.SemaphoreType.DMA
    return pl.pallas_call(
        functools.partial(fused_kernel, p),
        out_shape=(
            jax.ShapeDtypeStruct((n * p.quarter, p.cols), low),
            jax.ShapeDtypeStruct((p.width, p.row_count), low),
            jax.ShapeDtypeStruct((p.latents, p.row_count), low),
            jax.ShapeDtypeStruct((p.row_count, p.width), low),
            jax.ShapeDtypeStruct((p.row_count, p.latents), low),
        ),
        in_specs=[vmem] * 2 + [hbm] * 8,
        out_specs=(vmem,) * 5,
        scratch_shapes=[
            pltpu.VMEM(lengths.shape, jnp.int32),
            pltpu.VMEM(query_pos.shape, jnp.int32),
            pltpu.VMEM(resid.shape, low),
            pltpu.VMEM(enc_bias.shape, jnp.float32),
            pltpu.VMEM(dec_bias.shape, jnp.float32),
            pltpu.VMEM(out_weight.shape, low),
            pltpu.VMEM((p.width, p.latents), low),
            pltpu.VMEM((p.latents, p.width), low),
            pltpu.VMEM((p.shards * p.slots, 2 * p.head_dim), low),
            pltpu.VMEM((p.row_count, p.heads_local * p.head_dim), low),
            pltpu.VMEM((p.row_count, p.cols), low),
            pltpu.VMEM((n, p.half, p.cols), low),
            pltpu.VMEM((n, p.half, p.cols), low),
            pltpu.VMEM((n, highs, p.quarter, p.cols), low),
            pltpu.VMEM((n, p.grp, p.quarter, p.cols), low),
            pltpu.VMEM((p.row_count, p.width), low),
            pltpu.VMEM((p.row_count, p.latents), low),
            pltpu.VMEM((2, p.row_count, p.latents), low),
            pltpu.VMEM((2, n, p.half, p.latents), low),
            pltpu.VMEM((2, n, p.half, p.latents), low),
            pltpu.VMEM((2, n, highs, p.quarter, p.latents), low),
            pltpu.VMEM((n, p.quarter, p.latents), jnp.float32),
            pltpu.VMEM((p.row_count, p.width), low),
            pltpu.VMEM((n, ctxs, p.side, p.width), low),
            pltpu.VMEM((n, p.side, p.width), low),
            pltpu.VMEM((n, grps, p.piece, p.width), low),
            dma((8,)),
            dma((2, p.shards - 1)),
            dma((2, n, grps)),
            dma((2, n, ctxs, grps + 1)),
            dma((2, n)),
            dma((2, n, highs)),
            dma((2, n, grps)),
            dma((2, n, p.grp)),
            dma((2, n, ctxs, p.wid, p.grp)),
            dma((2, 2, n)),
            dma((2, 2, n, highs)),
            dma((2, 2, n, highs + 1)),
            dma((2, 2, n, highs)),
            dma((2, n, p.cuts, ctxs)),
            dma((2, n, p.cuts, grps)),
            dma((2, n, p.cuts, grps)),
            dma((2, n, p.cuts, ctxs, grps + 1)),
        ],
        compiler_params=pltpu.CompilerParams(
            collective_id=0, has_side_effects=True, vmem_limit_bytes=44 * 1024 * 1024
        ),
        name="fused",
    )(
        mine, cache,
        *(
            pltpu.with_memory_space_constraint(x, pltpu.HBM)
            for x in (lengths, query_pos, resid, enc_bias, dec_bias, out_weight, enc_weight, dec_weight)
        ),
    )


def grads_kernel(dec_step, enc_step, depth, block_t, lat_t, err, pgrad, layer_in, enc_out, dec_out, enc_sum, dec_sum, layer_out, dec_buf, enc_buf, sem):
    layer_out[...] = layer_in[...]
    jobs = [(0, i) for i in range(dec_out.shape[0] // dec_step)]
    jobs += [(1, i) for i in range(enc_out.shape[0] // enc_step)]
    started = []
    for k, (kind, i) in enumerate(jobs):
        x, y, out, buf, step = ((lat_t, err, dec_out, dec_buf, dec_step), (block_t, pgrad, enc_out, enc_buf, enc_step))[kind]
        slot = i % depth
        if i >= depth:
            started[k - depth].wait()
        rows = pl.ds(i * step, step)
        buf[slot] = jnp.dot(x[rows, :], y[...], preferred_element_type=jnp.float32).astype(jnp.bfloat16)
        copy = pltpu.make_async_copy(buf.at[slot], out.at[rows], sem.at[kind, slot])
        copy.start()
        started.append(copy)
    dec_sum[...] = jnp.sum(err[...].astype(jnp.float32), axis=0)
    enc_sum[...] = jnp.sum(pgrad[...].astype(jnp.float32), axis=0)
    for k, (kind, i) in enumerate(jobs):
        count = sum(1 for job in jobs if job[0] == kind)
        if i >= count - depth:
            started[k].wait()


def grads(block_t, lat_t, err, pgrad, layer_in):
    width, latents = block_t.shape[0], lat_t.shape[0]
    vmem = pl.BlockSpec(memory_space=pltpu.VMEM)
    hbm = pl.BlockSpec(memory_space=pltpu.HBM)
    dec_step, enc_step, depth = 1024, 256, 3
    enc, dec, enc_sum, dec_sum, layer_out = pl.pallas_call(
        functools.partial(grads_kernel, dec_step, enc_step, depth),
        out_shape=(
            jax.ShapeDtypeStruct((width, latents), jnp.bfloat16),
            jax.ShapeDtypeStruct((latents, width), jnp.bfloat16),
            jax.ShapeDtypeStruct((latents,), jnp.float32),
            jax.ShapeDtypeStruct((width,), jnp.float32),
            jax.ShapeDtypeStruct(layer_in.shape, layer_in.dtype),
        ),
        in_specs=[vmem] * 5,
        out_specs=(hbm, hbm, vmem, vmem, vmem),
        scratch_shapes=[
            pltpu.VMEM((depth, dec_step, width), jnp.bfloat16),
            pltpu.VMEM((depth, enc_step, latents), jnp.bfloat16),
            pltpu.SemaphoreType.DMA((2, depth)),
        ],
        compiler_params=pltpu.CompilerParams(vmem_limit_bytes=24 * 1024 * 1024),
        name="grads",
    )(block_t, lat_t, err, pgrad, layer_in)
    return layer_out, enc, enc_sum, dec, dec_sum


def attend(groups, query, keys, values, lengths, query_pos):
    seq_count, slot_count, kv_local, head_dim = keys.shape
    row_count, heads_local = query.shape[:2]
    group_size = heads_local // kv_local
    shards = groups.shards[0]
    pairs = seq_count * kv_local
    chunks = shards // pairs
    rows = row_count // seq_count // chunks
    pair = lax.axis_index(("grp", "ctx")) // chunks
    seq, head = pair // kv_local, lax.rem(pair, kv_local)
    row0 = seq * (row_count // seq_count) + lax.rem(lax.axis_index(("grp", "ctx")), chunks) * rows
    cache = jnp.concatenate([keys, values], axis=-1).transpose(0, 2, 1, 3)
    cache = cache.reshape(pairs, slot_count, 2 * head_dim)
    if chunks > 1:
        cache = jnp.repeat(cache, chunks, axis=0)
    cache = exchange(cache, *groups.shards, False, 0).reshape(shards * slot_count, 2 * head_dim)
    q = lax.dynamic_slice(query, (row0, head * group_size, 0), (rows, group_size, head_dim))
    live = lax.dynamic_index_in_dim(lengths, seq, 0, keepdims=False)
    before = jnp.arange(shards)[None, :] < jnp.arange(shards)[:, None]
    offset = jnp.sum(jnp.where(before, live[None, :], 0), axis=1)
    slot_ids = jnp.arange(slot_count, dtype=jnp.int32)
    key_pos = jnp.where(
        slot_ids[None, :] < live[:, None], offset[:, None] + slot_ids[None, :], jnp.int32(2**30)
    ).reshape(-1)
    position = lax.dynamic_slice_in_dim(query_pos, row0, rows, 0)
    visible = (key_pos[None, :] <= position[:, None])[:, None, :]
    scores = jnp.einsum(
        "rgd,td->rgt", q, cache[:, :head_dim], preferred_element_type=jnp.float32
    ) * HD ** (-0.5)
    peak = jnp.max(jnp.where(visible, scores, -1e30), axis=-1, keepdims=True)
    weights = jnp.where(visible, jnp.exp(scores - peak), 0.0)
    weight_sum = jnp.sum(weights, axis=-1, keepdims=True)
    weighted = jnp.einsum(
        "rgt,td->rgd", weights.astype(jnp.bfloat16), cache[:, head_dim:],
        preferred_element_type=jnp.float32,
    )
    mine = (weighted / weight_sum).astype(jnp.bfloat16).reshape(rows, group_size * head_dim)
    attention = exchange(mine, *groups.shards, True, 1)
    attention = attention.reshape(seq_count, kv_local, chunks, rows, group_size * head_dim)
    return attention.transpose(0, 2, 3, 1, 4).reshape(row_count, heads_local * head_dim)


def body(
    sizes,
    query,
    keys,
    values,
    lengths,
    query_pos,
    resid,
    out_weight,
    enc_weight,
    enc_bias,
    dec_weight,
    dec_bias,
):
    plan = Plan(sizes, query, keys, resid, enc_weight)
    if plan.fits():
        layer_out, block_t, lat_t, err, pgrad = fused(
            plan, query, keys, values, lengths, query_pos, resid, out_weight,
            enc_weight, enc_bias, dec_weight, dec_bias,
        )
        return grads(block_t, lat_t, err, pgrad, layer_out)
    groups = Groups(sizes)
    row_count = query.shape[0]
    shard_pos = lax.axis_index(("grp", "ctx"))
    attention = attend(groups, query, keys, values, lengths, query_pos)
    projected = jnp.dot(attention, out_weight, preferred_element_type=jnp.float32)
    mixed = scatter_sum(projected.astype(jnp.bfloat16), groups.wid, 2)
    layer_out = (mixed + resid.astype(jnp.float32)).astype(jnp.bfloat16)
    rows, cols = layer_out.shape
    wid_n = sizes["wid"]
    wide = exchange(layer_out, *groups.shards, True, 3)
    wide = wide.reshape(wid_n, -1, rows, cols).transpose(0, 2, 1, 3).reshape(wid_n, rows, -1)
    block = exchange(wide, *groups.wid, False, 4).reshape(row_count, -1)
    enc_part = jnp.dot(block, enc_weight, preferred_element_type=jnp.float32)
    preact = scatter_sum(enc_part.astype(jnp.bfloat16), groups.low, 5).astype(jnp.bfloat16)
    preact = scatter_sum(preact, groups.high, 6) + enc_bias
    my_latents = (jax.nn.softplus(4.0 * preact) * 0.25).astype(jnp.bfloat16)
    latents = gather_rows(gather_rows(my_latents, groups.high, 7), groups.low, 8)
    row_scale = row_count ** (-0.5)
    recon = jnp.dot(latents, dec_weight, preferred_element_type=jnp.float32)
    recon = scatter_sum(recon.astype(jnp.bfloat16), groups.shards, 9)
    piece_len = recon.shape[0]
    target = lax.dynamic_slice_in_dim(block, shard_pos * piece_len, piece_len, 0).astype(
        jnp.float32
    )
    scaled_error = ((recon + dec_bias - target) * row_scale).astype(jnp.bfloat16)
    error_all = gather_rows(scaled_error, groups.shards, 10)
    dec_bias_grad = jnp.sum(error_all, axis=0, dtype=jnp.float32)
    latent_part = lax.dot_general(
        error_all, dec_weight, (((1,), (1,)), ((), ())), preferred_element_type=jnp.float32
    )
    dec_grad = lax.dot_general(
        latents, error_all, (((0,), (0,)), ((), ())), preferred_element_type=jnp.float32
    )
    latent_grad = scatter_sum(latent_part.astype(jnp.bfloat16), groups.low, 11).astype(jnp.bfloat16)
    latent_grad = scatter_sum(latent_grad, groups.high, 12)
    my_grad = (latent_grad * jax.nn.sigmoid(4.0 * preact)).astype(jnp.bfloat16)
    preact_grad = gather_rows(gather_rows(my_grad, groups.high, 13), groups.low, 14)
    enc_grad = lax.dot_general(
        block, preact_grad, (((0,), (0,)), ((), ())), preferred_element_type=jnp.float32
    ).astype(jnp.bfloat16)
    enc_bias_grad = jnp.sum(preact_grad, axis=0, dtype=jnp.float32)
    return (layer_out, enc_grad, enc_bias_grad, dec_grad.astype(jnp.bfloat16), dec_bias_grad)


def solution(mesh):
    placed = (
        P(None, "wid", None),
        P(None, ("grp", "ctx"), "wid", None),
        P(None, ("grp", "ctx"), "wid", None),
        P(),
        P(),
        P("wid", ("grp", "ctx")),
        P("wid", ("grp", "ctx")),
        P("wid", ("grp", "ctx")),
        P(("grp", "ctx")),
        P(("grp", "ctx"), "wid"),
        P("wid"),
    )
    return jax.shard_map(
        functools.partial(body, dict(mesh.shape)),
        mesh=mesh,
        in_specs=placed,
        out_specs=(
            P("wid", ("grp", "ctx")),
            P("wid", ("grp", "ctx")),
            P(("grp", "ctx")),
            P(("grp", "ctx"), "wid"),
            P("wid"),
        ),
        check_vma=False,
    )
```

```python
import functools

import jax
import jax.numpy as jnp
from jax import lax
from jax.experimental import pallas as pl
from jax.experimental.pallas import tpu as pltpu
from jax.sharding import PartitionSpec as P

HD = 128
MESH = pl.DeviceIdType.MESH


def exchange_kernel(n, where, peer_id, gather, x_ref, out_ref, send_sem, recv_sem):
    me = where()
    peers = [lax.rem(me + step, n) for step in range(1, n)]
    barrier = pltpu.get_barrier_semaphore()
    for peer in peers:
        pl.semaphore_signal(barrier, inc=1, device_id=peer_id(peer), device_id_type=MESH)
    pl.semaphore_wait(barrier, n - 1)

    def copy_to(step, peer):
        return pltpu.make_async_remote_copy(
            src_ref=x_ref if gather else x_ref.at[peer],
            dst_ref=out_ref.at[me],
            send_sem=send_sem.at[step],
            recv_sem=recv_sem.at[me],
            device_id=peer_id(peer),
            device_id_type=MESH,
        )

    def copy_from(step, peer):
        return pltpu.make_async_remote_copy(
            src_ref=x_ref if gather else x_ref.at[peer],
            dst_ref=out_ref.at[peer],
            send_sem=send_sem.at[step],
            recv_sem=recv_sem.at[peer],
            device_id=peer_id(peer),
            device_id_type=MESH,
        )

    sends = [copy_to(step, peer) for step, peer in enumerate(peers)]
    for copy in sends:
        copy.start()
    out_ref[me] = x_ref[...] if gather else x_ref[me]
    for step, peer in enumerate(peers):
        copy_from(step, peer).wait_recv()
    for copy in sends:
        copy.wait_send()


def exchange(x, n, where, peer_id, gather, number):
    block = x.shape if gather else x.shape[1:]
    return pl.pallas_call(
        functools.partial(exchange_kernel, n, where, peer_id, gather),
        out_shape=jax.ShapeDtypeStruct((n,) + block, x.dtype),
        in_specs=[pl.BlockSpec(memory_space=pltpu.VMEM)],
        out_specs=pl.BlockSpec(memory_space=pltpu.VMEM),
        scratch_shapes=[pltpu.SemaphoreType.DMA((n,)), pltpu.SemaphoreType.DMA((n,))],
        compiler_params=pltpu.CompilerParams(
            collective_id=number, has_side_effects=True, vmem_limit_bytes=24 * 1024 * 1024
        ),
        name="exchange%d" % number,
    )(x)


class Groups:
    def __init__(self, sizes):
        ctx_n = sizes["ctx"]
        self.shards = (
            sizes["grp"] * ctx_n,
            lambda: lax.axis_index("grp") * ctx_n + lax.axis_index("ctx"),
            lambda p: {"grp": p // ctx_n, "ctx": lax.rem(p, ctx_n)},
        )
        self.wid = (sizes["wid"], lambda: lax.axis_index("wid"), lambda p: {"wid": p})
        self.low = (
            2,
            lambda: lax.rem(lax.axis_index("wid"), 2),
            lambda p: {"wid": (lax.axis_index("wid") // 2) * 2 + p},
        )
        self.high = (
            sizes["wid"] // 2,
            lambda: lax.axis_index("wid") // 2,
            lambda p: {"wid": p * 2 + lax.rem(lax.axis_index("wid"), 2)},
        )


def scatter_sum(x, group, number):
    n = group[0]
    parts = exchange(x.reshape((n, x.shape[0] // n) + x.shape[1:]), *group, False, number)
    return jnp.sum(parts.astype(jnp.float32), axis=0)


def gather_rows(x, group, number):
    whole = exchange(x, *group, True, number)
    return whole.reshape((whole.shape[0] * whole.shape[1],) + whole.shape[2:])


def rows_at(start, size):
    return pl.ds(pl.multiple_of(start, 16), size)


def cols_at(start, size):
    return pl.ds(pl.multiple_of(start, 128), size)


def partners(me, n):
    if n == 2:
        to = [1 - me]
        return to, to
    if n == 4:
        near = me + 1 - 2 * lax.rem(me, 2)
        to = [near, lax.rem(me + 2, 4), lax.rem(near + 2, 4)]
        return to, to
    return (
        [lax.rem(me + k, n) for k in range(1, n)],
        [lax.rem(me + n - k, n) for k in range(1, n)],
    )


class Plan:
    def __init__(self, sizes, query, keys, resid, enc_weight):
        self.grp, self.ctx, self.wid = sizes["grp"], sizes["ctx"], sizes["wid"]
        self.high = self.wid // 2
        self.shards = self.grp * self.ctx
        self.row_count, self.heads_local, self.head_dim = query.shape
        self.seqs, self.slots, self.kv_local = keys.shape[:3]
        self.heads = self.heads_local // self.kv_local
        self.width, self.latents = enc_weight.shape
        self.cols = resid.shape[1]
        self.streams = 2
        self.rows = self.row_count // self.streams
        self.half = self.rows // 2
        self.quarter = self.rows // self.wid
        self.side = self.rows // self.ctx
        self.piece = self.side // self.grp
        self.cuts = 2

    def fits(self):
        return (
            self.wid % 2 == 0
            and self.grp == self.wid == self.seqs
            and self.ctx == self.kv_local
            and self.ctx > 1
            and self.rows % (16 * self.wid) == 0
            and self.rows % (16 * self.shards) == 0
            and self.cols % 128 == 0
            and self.cols * self.ctx == self.width
            and self.width % (128 * self.cuts) == 0
            and self.latents % 512 == 0
            and self.head_dim % 128 == 0
            and self.heads % 2 == 0
        )


def fused_kernel(
    plan, query, cache, len_hbm, pos_hbm, resid_hbm, eb_hbm, db_hbm, out_hbm, enc_hbm, dec_hbm,
    layer_out, block_t, dec_grad, dec_sum, pgrad,
    lat_t, err, lengths, query_pos, resid, enc_bias, dec_bias, out_w, enc_w, dec_w, kv, att, proj, opair_in, opair_sum, ohigh_in, zin, block, lat,
    part, pair_in, pair_sum, high_in, factor, recon, side_in, side_sum, piece_in,
    load_sem, kv_sem, att_sem, att_cross, opair_sem, ohigh_sem, lo_sem, blk_sem, blk_cross,
    pair_sem, high_sem, gather_sem, relay_sem, side_sem, piece_sem, spread_sem, cross_sem,
):
    p = plan
    g, c, w = lax.axis_index("grp"), lax.axis_index("ctx"), lax.axis_index("wid")
    low, high = lax.rem(w, 2), w // 2
    partner = {"wid": w + 1 - 2 * low}
    highs, highs_from = partners(high, p.high)
    ctxs, ctxs_from = partners(c, p.ctx)
    grps, grps_from = partners(g, p.grp)
    to_high = lambda h: {"wid": h * 2 + low}
    to_ctx = lambda q: {"ctx": q}
    to_grp = lambda q: {"grp": q}
    others = [(1 - low, high)] + [(low, h) for h in highs_from] + [(1 - low, h) for h in highs_from]
    shard_to = [(q, r) for q in [g] + grps for r in [c] + ctxs][1:]
    shard_from = [(q, r) for q in [g] + grps_from for r in [c] + ctxs_from][1:]

    enc_step = 512
    enc_steps = p.latents // enc_step

    def load(src, dst, index):
        copy = pltpu.make_async_copy(src, dst, load_sem.at[index])
        copy.start()
        return copy

    barrier = pltpu.get_barrier_semaphore()
    greeted = [{"grp": q, "ctx": r} for q, r in shard_to]
    greeted += [{"wid": hi * 2 + lo} for lo, hi in others]
    for peer in greeted:
        pl.semaphore_signal(barrier, inc=1, device_id=peer, device_id_type=MESH)
    small_loads = [
        load(src, dst, 3 + k)
        for k, (src, dst) in enumerate(
            [(len_hbm, lengths), (pos_hbm, query_pos), (resid_hbm, resid), (eb_hbm, enc_bias), (db_hbm, dec_bias)]
        )
    ]
    out_load = load(out_hbm, out_w, 0)
    enc_load = load(enc_hbm, enc_w, 1)
    dec_load = load(dec_hbm, dec_w, 2)
    pl.semaphore_wait(barrier, len(greeted))

    pending = []

    def send(src, dst, sem, index, peer, to_index=None, when=None):
        copy = pltpu.make_async_remote_copy(
            src_ref=src, dst_ref=dst, send_sem=sem.at[(0,) + index],
            recv_sem=sem.at[(1,) + (index if to_index is None else to_index)],
            device_id=peer, device_id_type=MESH,
        )
        if when is None:
            copy.start()
        else:
            pl.when(when)(lambda: copy.start())
        pending.append((copy, when))

    def arrived(ref, sem, index):
        pltpu.make_async_remote_copy(
            src_ref=ref, dst_ref=ref, send_sem=sem.at[(0,) + index], recv_sem=sem.at[(1,) + index],
            device_id=partner, device_id_type=MESH,
        ).wait_recv()

    def quarter_row(t, lo, hi):
        return t * p.rows + (lo * p.high + hi) * p.quarter

    def piece_row(t, q, r):
        return t * p.rows + q * p.side + r * p.piece

    def shard(q, r):
        return q * p.ctx + r

    def loop(count, body):
        def step(i, carry):
            body(pl.multiple_of(i * 16, 16))
            return carry

        lax.fori_loop(0, count // 16, step, 0)

    def cache_send():
        for k, (q, r) in reversed(list(enumerate(shard_to))):
            send(
                cache.at[shard(q, r)], kv.at[rows_at(shard(g, c) * p.slots, p.slots)],
                kv_sem, (k,), {"grp": q, "ctx": r},
            )
        kv[rows_at(shard(g, c) * p.slots, p.slots)] = cache[shard(g, c)]

    def cache_wait():
        for k, (q, r) in enumerate(shard_from):
            arrived(kv.at[rows_at(shard(q, r) * p.slots, p.slots)], kv_sem, (k,))

    def att_at(t, q, r):
        return att.at[
            rows_at(quarter_row(t, lax.rem(q, 2), q // 2), p.quarter),
            cols_at(r * p.heads * p.head_dim, p.heads * p.head_dim),
        ]

    def key_positions():
        live = lengths[pl.ds(g, 1), :]
        slot = lax.broadcasted_iota(jnp.int32, (1, p.shards * p.slots), 1)
        key = jnp.full((1, p.shards * p.slots), 2**30, jnp.int32)
        offset = jnp.zeros((1, 1), jnp.int32)
        for b in range(p.shards):
            count = live[:, b : b + 1]
            own = slot - b * p.slots
            key = jnp.where((own >= 0) & (own < p.slots) & (own < count), offset + own, key)
            offset = offset + count
        return key

    def row_positions(t):
        shape = (2 * p.quarter, p.row_count)
        row = lax.broadcasted_iota(jnp.int32, shape, 0)
        wanted = lax.rem(row, p.quarter) + (g * (p.row_count // p.seqs) + t * p.quarter)
        here = lax.broadcasted_iota(jnp.int32, shape, 1) == wanted
        values = jnp.where(here, query_pos[...].reshape(1, -1).astype(jnp.float32), 0.0)
        return jnp.sum(values, axis=1, keepdims=True).astype(jnp.int32)

    def attend_rows(t):
        two = 2 * p.quarter
        visible = key_positions() <= row_positions(t)
        mine = att_at(t, g, c)
        for i in range(p.heads // 2):
            scores = lax.dot_general(
                query[t, pl.ds(i * two, two)], kv[:, : p.head_dim], (((1,), (1,)), ((), ())),
                preferred_element_type=jnp.float32,
            ) * p.head_dim ** (-0.5)
            peak = jnp.max(jnp.where(visible, scores, -1e30), axis=-1, keepdims=True)
            weights = jnp.where(visible, jnp.exp(scores - peak), 0.0)
            total = jnp.sum(weights, axis=-1, keepdims=True)
            weighted = jnp.dot(
                weights.astype(jnp.bfloat16), kv[:, p.head_dim :], preferred_element_type=jnp.float32
            )
            out = (weighted / total).astype(jnp.bfloat16)
            for j in range(2):
                mine[:, pl.ds((2 * i + j) * p.head_dim, p.head_dim)] = out[j * p.quarter : (j + 1) * p.quarter]
        for k, q in enumerate(grps):
            send(mine, mine, att_sem, (t, k), to_grp(q))
        for i, r in enumerate(ctxs):
            send(mine, mine, att_cross, (t, i, 0), to_ctx(r))

    def att_relay(t):
        for k, q in enumerate(grps_from):
            theirs = att_at(t, q, c)
            arrived(theirs, att_sem, (t, k))
            for i, r in enumerate(ctxs):
                send(theirs, theirs, att_cross, (t, i, k + 1), to_ctx(r))

    def project(t):
        for i, r in enumerate(ctxs_from):
            for k, q in enumerate([g] + grps_from):
                arrived(att_at(t, q, r), att_cross, (t, i, k))
        if t == 0:
            out_load.wait()
        rows = pl.ds(t * p.rows, p.rows)
        proj[rows] = jnp.dot(att[rows], out_w[...], preferred_element_type=jnp.float32).astype(jnp.bfloat16)
        send(
            proj.at[rows_at(t * p.rows + (1 - low) * p.half, p.half)], opair_in.at[t], opair_sem, (t,), partner
        )

    def project_add(t):
        arrived(opair_in.at[t], opair_sem, (t,))

        def body(r):
            mine = proj[rows_at(t * p.rows + low * p.half + r, 16)].astype(jnp.float32)
            opair_sum[t, pl.ds(r, 16)] = (mine + opair_in[t, pl.ds(r, 16)].astype(jnp.float32)).astype(jnp.bfloat16)

        loop(p.half, body)
        for s, h in enumerate(highs):
            send(opair_sum.at[t, rows_at(h * p.quarter, p.quarter)], ohigh_in.at[t, s], ohigh_sem, (t, s), to_high(h))

    def layer(t):
        for s in range(len(highs)):
            arrived(ohigh_in.at[t, s], ohigh_sem, (t, s))

        def body(r):
            total = opair_sum[t, rows_at(high * p.quarter + r, 16)].astype(jnp.float32)
            for s in range(len(highs)):
                total = total + ohigh_in[t, s, pl.ds(r, 16)].astype(jnp.float32)
            rows = rows_at(t * p.quarter + r, 16)
            value = (total + resid[rows].astype(jnp.float32)).astype(jnp.bfloat16)
            layer_out[rows] = value
            zin[t, g, pl.ds(r, 16)] = value

        loop(p.quarter, body)
        for k, q in enumerate(grps):
            send(zin.at[t, g], zin.at[t, g], lo_sem, (t, k), to_grp(q))

    def block_at(t, lo, hi, r):
        return block.at[rows_at(quarter_row(t, lo, hi), p.quarter), cols_at(r * p.cols, p.cols)]

    def block_relay(t):
        mine = block_at(t, low, high, c)
        for k, q in enumerate([g] + grps_from):
            if k:
                arrived(zin.at[t, q], lo_sem, (t, k - 1))
            owned, away = w == q, w != q

            @pl.when(owned)
            def _(q=q):
                mine[...] = zin[t, q]

            for i, r in enumerate(ctxs):
                send(mine, mine, blk_cross, (t, i, 0, k), to_ctx(r), (t, i, 0, 0), owned)
            send(zin.at[t, q], mine, blk_sem, (t, k), {"wid": q}, (t, w), away)

    def block_spread(t):
        for j, (lo, hi) in enumerate(others):
            theirs = block_at(t, lo, hi, c)
            arrived(theirs, blk_sem, (t, hi * 2 + lo))
            for i, r in enumerate(ctxs):
                send(theirs, theirs, blk_cross, (t, i, j + 1, 0), to_ctx(r))

    def block_wait(t):
        for i, r in enumerate(ctxs_from):
            for j, (lo, hi) in enumerate([(low, high)] + others):
                arrived(block_at(t, lo, hi, r), blk_cross, (t, i, j, 0))

    def pair_send(k, t):
        there = part.at[k, rows_at(t * p.rows + (1 - low) * p.half, p.half)]
        send(there, pair_in.at[k, t], pair_sem, (k, t), partner)

    def pair_add(k, t):
        arrived(pair_in.at[k, t], pair_sem, (k, t))

        def body(r):
            mine = part[k, rows_at(t * p.rows + low * p.half + r, 16)].astype(jnp.float32)
            pair_sum[k, t, pl.ds(r, 16)] = (mine + pair_in[k, t, pl.ds(r, 16)].astype(jnp.float32)).astype(jnp.bfloat16)

        loop(p.half, body)
        for s, h in enumerate(highs):
            send(pair_sum.at[k, t, rows_at(h * p.quarter, p.quarter)], high_in.at[k, t, s], high_sem, (k, t, s), to_high(h))

    def high_sum(k, t, r):
        total = pair_sum[k, t, rows_at(high * p.quarter + r, 16)].astype(jnp.float32)
        for s in range(len(highs)):
            total = total + high_in[k, t, s, pl.ds(r, 16)].astype(jnp.float32)
        return total

    def publish(k, t, out):
        mine = out.at[rows_at(quarter_row(t, low, high), p.quarter)]
        for s, h in enumerate(highs):
            send(mine, mine, gather_sem, (k, t, s + 1), to_high(h))
        send(mine, mine, gather_sem, (k, t, 0), partner)

    def activate(t):
        for s in range(len(highs)):
            arrived(high_in.at[0, t, s], high_sem, (0, t, s))

        def body(r):
            z = 4.0 * (high_sum(0, t, r) + enc_bias[...].reshape(1, -1))
            e = jnp.exp(-jnp.abs(z))
            lat[rows_at(quarter_row(t, low, high) + r, 16)] = (
                (jnp.maximum(z, 0.0) + jnp.log1p(e)) * 0.25
            ).astype(jnp.bfloat16)
            factor[t, pl.ds(r, 16)] = jnp.where(z >= 0.0, 1.0, e) / (1.0 + e)

        loop(p.quarter, body)
        publish(0, t, lat)

    def cotangent(t):
        for s in range(len(highs)):
            arrived(high_in.at[1, t, s], high_sem, (1, t, s))

        def body(r):
            pgrad[rows_at(quarter_row(t, low, high) + r, 16)] = (
                high_sum(1, t, r) * factor[t, pl.ds(r, 16)]
            ).astype(jnp.bfloat16)

        loop(p.quarter, body)
        publish(1, t, pgrad)

    def relay(k, t, out):
        for s, h in enumerate(highs_from):
            theirs = out.at[rows_at(quarter_row(t, low, h), p.quarter)]
            arrived(theirs, gather_sem, (k, t, s + 1))
            send(theirs, theirs, relay_sem, (k, t, s), partner)

    def collected(k, t, out):
        arrived(out.at[rows_at(quarter_row(t, 1 - low, high), p.quarter)], gather_sem, (k, t, 0))
        for s, h in enumerate(highs_from):
            arrived(out.at[rows_at(quarter_row(t, 1 - low, h), p.quarter)], relay_sem, (k, t, s))

    def encode(t):
        block_wait(t)
        if t == 0:
            enc_load.wait()
        rows = pl.ds(t * p.rows, p.rows)

        def step(j, carry):
            cols = cols_at(j * enc_step, enc_step)
            part[0, rows, cols] = jnp.dot(
                block[rows, :], enc_w[:, cols], preferred_element_type=jnp.float32
            ).astype(jnp.bfloat16)
            return carry

        lax.fori_loop(0, enc_steps, step, 0)
        pair_send(0, t)

    cut = p.width // p.cuts

    def decode(t):
        collected(0, t, lat)
        if t == 0:
            dec_load.wait()
        rows = pl.ds(t * p.rows, p.rows)
        for j in range(p.cuts):
            cols = pl.ds(j * cut, cut)
            recon[rows, cols] = jnp.dot(
                lat[rows, :], dec_w[:, cols], preferred_element_type=jnp.float32
            ).astype(jnp.bfloat16)
            for s, q in enumerate(ctxs):
                send(
                    recon.at[rows_at(piece_row(t, q, 0), p.side), cols], side_in.at[t, s, :, cols],
                    side_sem, (t, j, s), to_ctx(q),
                )

    def side_add(t):
        for j in range(p.cuts):
            cols = pl.ds(j * cut, cut)
            for s in range(len(ctxs)):
                arrived(side_in.at[t, s, :, cols], side_sem, (t, j, s))
            total = recon[rows_at(piece_row(t, c, 0), p.side), cols].astype(jnp.float32)
            for s in range(len(ctxs)):
                total = total + side_in[t, s, :, cols].astype(jnp.float32)
            side_sum[t, :, cols] = total.astype(jnp.bfloat16)
            for s, q in enumerate(grps):
                send(
                    side_sum.at[t, rows_at(q * p.piece, p.piece), cols], piece_in.at[t, s, :, cols],
                    piece_sem, (t, j, s), to_grp(q),
                )

    def err_at(t, q, r, cols):
        return err.at[rows_at(piece_row(t, q, r), p.piece), cols]

    def error(t):
        for j in range(p.cuts):
            cols = pl.ds(j * cut, cut)
            for s in range(len(grps)):
                arrived(piece_in.at[t, s, :, cols], piece_sem, (t, j, s))
            total = side_sum[t, rows_at(g * p.piece, p.piece), cols].astype(jnp.float32)
            for s in range(len(grps)):
                total = total + piece_in[t, s, :, cols].astype(jnp.float32)
            rows = rows_at(piece_row(t, c, g), p.piece)
            wanted = block[rows, cols].astype(jnp.float32)
            err[rows, cols] = ((total + dec_bias[cols].reshape(1, -1) - wanted) * p.row_count ** (-0.5)).astype(jnp.bfloat16)
            mine = err_at(t, c, g, cols)
            for s, q in enumerate(grps):
                send(mine, mine, spread_sem, (t, j, s), to_grp(q))
            for s, q in enumerate(ctxs):
                send(mine, mine, cross_sem, (t, j, s, 0), to_ctx(q))

    def error_relay(t):
        for j in range(p.cuts):
            cols = pl.ds(j * cut, cut)
            for i, r in enumerate(grps_from):
                theirs = err_at(t, c, r, cols)
                arrived(theirs, spread_sem, (t, j, i))
                for s, q in enumerate(ctxs):
                    send(theirs, theirs, cross_sem, (t, j, s, i + 1), to_ctx(q))

    def back(t):
        for j in range(p.cuts):
            for s, q in enumerate(ctxs_from):
                for i, r in enumerate([g] + grps_from):
                    arrived(err_at(t, q, r, pl.ds(j * cut, cut)), cross_sem, (t, j, s, i))
        rows = pl.ds(t * p.rows, p.rows)

        def step(j, carry):
            cols = pl.ds(pl.multiple_of(j * enc_step, enc_step), enc_step)
            part[1, rows, cols] = lax.dot_general(
                err[rows, :], dec_w[cols, :], (((1,), (1,)), ((), ())), preferred_element_type=jnp.float32
            ).astype(jnp.bfloat16)
            return carry

        lax.fori_loop(0, enc_steps, step, 0)
        pair_send(1, t)

    out_step = 512

    def outer(j):
        rows = pl.ds(j * out_step, out_step)
        dec_grad[rows] = jnp.dot(lat_t[rows, :], err[...], preferred_element_type=jnp.float32).astype(jnp.bfloat16)

    def error_sum():
        dec_sum[...] = jnp.sum(err[...].astype(jnp.float32), axis=0)

    def outers(first, last):
        for j in range(first * (p.latents // out_step) // 6, last * (p.latents // out_step) // 6):
            outer(j)

    def turn(src, dst, t, count):
        rows = pl.ds(t * p.rows, p.rows)

        def step(j, carry):
            cols = cols_at(j * 256, 256)
            dst[cols, rows] = src[rows, cols].T
            return carry

        lax.fori_loop(0, count // 256, step, 0)

    cache_send()
    for copy in small_loads:
        copy.wait()
    cache_wait()
    stages = [
        lambda: attend_rows(0),
        lambda: attend_rows(1),
        lambda: att_relay(0),
        lambda: project(0),
        lambda: att_relay(1),
        lambda: project_add(0),
        lambda: project(1),
        lambda: layer(0),
        lambda: project_add(1),
        lambda: block_relay(0),
        lambda: layer(1),
        lambda: block_spread(0),
        lambda: block_relay(1),
        lambda: block_spread(1),
        lambda: encode(0),
        lambda: pair_add(0, 0),
        lambda: encode(1),
        lambda: pair_add(0, 1),
        lambda: turn(block, block_t, 0, p.width),
        lambda: turn(block, block_t, 1, p.width),
        lambda: activate(0),
        lambda: activate(1),
        lambda: relay(0, 0, lat),
        lambda: decode(0),
        lambda: turn(lat, lat_t, 0, p.latents),
        lambda: relay(0, 1, lat),
        lambda: side_add(0),
        lambda: decode(1),
        lambda: error(0),
        lambda: side_add(1),
        lambda: turn(lat, lat_t, 1, p.latents),
        lambda: error_relay(0),
        lambda: error(1),
        lambda: back(0),
        lambda: error_relay(1),
        lambda: pair_add(1, 0),
        lambda: back(1),
        lambda: pair_add(1, 1),
        lambda: cotangent(0),
        lambda: outers(0, 3),
        lambda: cotangent(1),
        lambda: outers(3, 6),
        error_sum,
        lambda: relay(1, 0, pgrad),
        lambda: relay(1, 1, pgrad),
        lambda: collected(1, 0, pgrad),
        lambda: collected(1, 1, pgrad),
    ]
    for stage in stages:
        stage()
    for copy, when in pending:
        if when is None:
            copy.wait_send()
        else:
            pl.when(when)(lambda copy=copy: copy.wait_send())


def fused(plan, query, keys, values, lengths, query_pos, resid, out_weight, enc_weight, enc_bias, dec_weight, dec_bias):
    p = plan
    low = jnp.bfloat16
    g, c = lax.axis_index("grp"), lax.axis_index("ctx")
    cache = jnp.concatenate([keys, values], axis=-1).transpose(0, 2, 1, 3)
    cache = cache.reshape(p.shards, p.slots, 2 * p.head_dim)
    seq_rows = p.row_count // p.seqs
    mine = lax.dynamic_slice(query, (g * seq_rows, c * p.heads, 0), (seq_rows, p.heads, p.head_dim))
    mine = mine.reshape(p.streams, p.quarter, p.heads, p.head_dim).transpose(0, 2, 1, 3)
    mine = mine.reshape(p.streams, p.heads * p.quarter, p.head_dim)

    vmem = pl.BlockSpec(memory_space=pltpu.VMEM)
    hbm = pl.BlockSpec(memory_space=pltpu.HBM)
    n, highs, ctxs, grps = p.streams, p.high - 1, p.ctx - 1, p.grp - 1
    dma = pltpu.SemaphoreType.DMA
    return pl.pallas_call(
        functools.partial(fused_kernel, p),
        out_shape=(
            jax.ShapeDtypeStruct((n * p.quarter, p.cols), low),
            jax.ShapeDtypeStruct((p.width, p.row_count), low),
            jax.ShapeDtypeStruct((p.latents, p.width), low),
            jax.ShapeDtypeStruct((p.width,), jnp.float32),
            jax.ShapeDtypeStruct((p.row_count, p.latents), low),
        ),
        in_specs=[vmem] * 2 + [hbm] * 8,
        out_specs=(vmem,) * 5,
        scratch_shapes=[
            pltpu.VMEM((p.latents, p.row_count), low),
            pltpu.VMEM((p.row_count, p.width), low),
            pltpu.VMEM(lengths.shape, jnp.int32),
            pltpu.VMEM(query_pos.shape, jnp.int32),
            pltpu.VMEM(resid.shape, low),
            pltpu.VMEM(enc_bias.shape, jnp.float32),
            pltpu.VMEM(dec_bias.shape, jnp.float32),
            pltpu.VMEM(out_weight.shape, low),
            pltpu.VMEM((p.width, p.latents), low),
            pltpu.VMEM((p.latents, p.width), low),
            pltpu.VMEM((p.shards * p.slots, 2 * p.head_dim), low),
            pltpu.VMEM((p.row_count, p.heads_local * p.head_dim), low),
            pltpu.VMEM((p.row_count, p.cols), low),
            pltpu.VMEM((n, p.half, p.cols), low),
            pltpu.VMEM((n, p.half, p.cols), low),
            pltpu.VMEM((n, highs, p.quarter, p.cols), low),
            pltpu.VMEM((n, p.grp, p.quarter, p.cols), low),
            pltpu.VMEM((p.row_count, p.width), low),
            pltpu.VMEM((p.row_count, p.latents), low),
            pltpu.VMEM((2, p.row_count, p.latents), low),
            pltpu.VMEM((2, n, p.half, p.latents), low),
            pltpu.VMEM((2, n, p.half, p.latents), low),
            pltpu.VMEM((2, n, highs, p.quarter, p.latents), low),
            pltpu.VMEM((n, p.quarter, p.latents), jnp.float32),
            pltpu.VMEM((p.row_count, p.width), low),
            pltpu.VMEM((n, ctxs, p.side, p.width), low),
            pltpu.VMEM((n, p.side, p.width), low),
            pltpu.VMEM((n, grps, p.piece, p.width), low),
            dma((8,)),
            dma((2, p.shards - 1)),
            dma((2, n, grps)),
            dma((2, n, ctxs, grps + 1)),
            dma((2, n)),
            dma((2, n, highs)),
            dma((2, n, grps)),
            dma((2, n, p.grp)),
            dma((2, n, ctxs, p.wid, p.grp)),
            dma((2, 2, n)),
            dma((2, 2, n, highs)),
            dma((2, 2, n, highs + 1)),
            dma((2, 2, n, highs)),
            dma((2, n, p.cuts, ctxs)),
            dma((2, n, p.cuts, grps)),
            dma((2, n, p.cuts, grps)),
            dma((2, n, p.cuts, ctxs, grps + 1)),
        ],
        compiler_params=pltpu.CompilerParams(
            collective_id=0, has_side_effects=True, vmem_limit_bytes=40 * 1024 * 1024
        ),
        name="fused",
    )(
        mine, cache,
        *(
            pltpu.with_memory_space_constraint(x, pltpu.HBM)
            for x in (lengths, query_pos, resid, enc_bias, dec_bias, out_weight, enc_weight, dec_weight)
        ),
    )


def grads_kernel(
    step, depth, block_t, dec_in, dec_sum_in, pgrad, layer_in, enc_out, dec_out, enc_sum, dec_sum, layer_out, buf, sem, dec_sem,
):
    dec_rows = dec_in.shape[0] // 2
    halves = [
        pltpu.make_async_copy(
            dec_in.at[pl.ds(i * dec_rows, dec_rows)], dec_out.at[pl.ds(i * dec_rows, dec_rows)], dec_sem.at[i]
        )
        for i in range(2)
    ]
    for copy in halves:
        copy.start()
    count = enc_out.shape[0] // step
    started = []
    for i in range(count):
        slot = i % depth
        if i >= depth:
            started[i - depth].wait()
        rows = pl.ds(i * step, step)
        buf[slot] = jnp.dot(block_t[rows, :], pgrad[...], preferred_element_type=jnp.float32).astype(jnp.bfloat16)
        copy = pltpu.make_async_copy(buf.at[slot], enc_out.at[rows], sem.at[slot])
        copy.start()
        started.append(copy)
    layer_out[...] = layer_in[...]
    dec_sum[...] = dec_sum_in[...]
    enc_sum[...] = jnp.sum(pgrad[...].astype(jnp.float32), axis=0)
    for copy in started[max(0, count - depth) :] + halves:
        copy.wait()


def grads(block_t, dec_grad, dec_bias_grad, pgrad, layer_in):
    width, latents = block_t.shape[0], pgrad.shape[1]
    vmem = pl.BlockSpec(memory_space=pltpu.VMEM)
    hbm = pl.BlockSpec(memory_space=pltpu.HBM)
    step, depth = 256, 5
    enc, dec, enc_sum, dec_sum, layer_out = pl.pallas_call(
        functools.partial(grads_kernel, step, depth),
        out_shape=(
            jax.ShapeDtypeStruct((width, latents), jnp.bfloat16),
            jax.ShapeDtypeStruct((latents, width), jnp.bfloat16),
            jax.ShapeDtypeStruct((latents,), jnp.float32),
            jax.ShapeDtypeStruct((width,), jnp.float32),
            jax.ShapeDtypeStruct(layer_in.shape, layer_in.dtype),
        ),
        in_specs=[vmem] * 5,
        out_specs=(hbm, hbm, vmem, vmem, vmem),
        scratch_shapes=[
            pltpu.VMEM((depth, step, latents), jnp.bfloat16),
            pltpu.SemaphoreType.DMA((depth,)),
            pltpu.SemaphoreType.DMA((2,)),
        ],
        compiler_params=pltpu.CompilerParams(vmem_limit_bytes=16 * 1024 * 1024),
        name="grads",
    )(block_t, dec_grad, dec_bias_grad, pgrad, layer_in)
    return layer_out, enc, enc_sum, dec, dec_sum


def attend(groups, query, keys, values, lengths, query_pos):
    seq_count, slot_count, kv_local, head_dim = keys.shape
    row_count, heads_local = query.shape[:2]
    group_size = heads_local // kv_local
    shards = groups.shards[0]
    pairs = seq_count * kv_local
    chunks = shards // pairs
    rows = row_count // seq_count // chunks
    pair = lax.axis_index(("grp", "ctx")) // chunks
    seq, head = pair // kv_local, lax.rem(pair, kv_local)
    row0 = seq * (row_count // seq_count) + lax.rem(lax.axis_index(("grp", "ctx")), chunks) * rows
    cache = jnp.concatenate([keys, values], axis=-1).transpose(0, 2, 1, 3)
    cache = cache.reshape(pairs, slot_count, 2 * head_dim)
    if chunks > 1:
        cache = jnp.repeat(cache, chunks, axis=0)
    cache = exchange(cache, *groups.shards, False, 0).reshape(shards * slot_count, 2 * head_dim)
    q = lax.dynamic_slice(query, (row0, head * group_size, 0), (rows, group_size, head_dim))
    live = lax.dynamic_index_in_dim(lengths, seq, 0, keepdims=False)
    before = jnp.arange(shards)[None, :] < jnp.arange(shards)[:, None]
    offset = jnp.sum(jnp.where(before, live[None, :], 0), axis=1)
    slot_ids = jnp.arange(slot_count, dtype=jnp.int32)
    key_pos = jnp.where(
        slot_ids[None, :] < live[:, None], offset[:, None] + slot_ids[None, :], jnp.int32(2**30)
    ).reshape(-1)
    position = lax.dynamic_slice_in_dim(query_pos, row0, rows, 0)
    visible = (key_pos[None, :] <= position[:, None])[:, None, :]
    scores = jnp.einsum(
        "rgd,td->rgt", q, cache[:, :head_dim], preferred_element_type=jnp.float32
    ) * HD ** (-0.5)
    peak = jnp.max(jnp.where(visible, scores, -1e30), axis=-1, keepdims=True)
    weights = jnp.where(visible, jnp.exp(scores - peak), 0.0)
    weight_sum = jnp.sum(weights, axis=-1, keepdims=True)
    weighted = jnp.einsum(
        "rgt,td->rgd", weights.astype(jnp.bfloat16), cache[:, head_dim:],
        preferred_element_type=jnp.float32,
    )
    mine = (weighted / weight_sum).astype(jnp.bfloat16).reshape(rows, group_size * head_dim)
    attention = exchange(mine, *groups.shards, True, 1)
    attention = attention.reshape(seq_count, kv_local, chunks, rows, group_size * head_dim)
    return attention.transpose(0, 2, 3, 1, 4).reshape(row_count, heads_local * head_dim)


def body(
    sizes,
    query,
    keys,
    values,
    lengths,
    query_pos,
    resid,
    out_weight,
    enc_weight,
    enc_bias,
    dec_weight,
    dec_bias,
):
    plan = Plan(sizes, query, keys, resid, enc_weight)
    if plan.fits():
        layer_out, block_t, dec_grad, dec_bias_grad, pgrad = fused(
            plan, query, keys, values, lengths, query_pos, resid, out_weight,
            enc_weight, enc_bias, dec_weight, dec_bias,
        )
        return grads(block_t, dec_grad, dec_bias_grad, pgrad, layer_out)
    groups = Groups(sizes)
    row_count = query.shape[0]
    shard_pos = lax.axis_index(("grp", "ctx"))
    attention = attend(groups, query, keys, values, lengths, query_pos)
    projected = jnp.dot(attention, out_weight, preferred_element_type=jnp.float32)
    mixed = scatter_sum(projected.astype(jnp.bfloat16), groups.wid, 2)
    layer_out = (mixed + resid.astype(jnp.float32)).astype(jnp.bfloat16)
    rows, cols = layer_out.shape
    wid_n = sizes["wid"]
    wide = exchange(layer_out, *groups.shards, True, 3)
    wide = wide.reshape(wid_n, -1, rows, cols).transpose(0, 2, 1, 3).reshape(wid_n, rows, -1)
    block = exchange(wide, *groups.wid, False, 4).reshape(row_count, -1)
    enc_part = jnp.dot(block, enc_weight, preferred_element_type=jnp.float32)
    preact = scatter_sum(enc_part.astype(jnp.bfloat16), groups.low, 5).astype(jnp.bfloat16)
    preact = scatter_sum(preact, groups.high, 6) + enc_bias
    my_latents = (jax.nn.softplus(4.0 * preact) * 0.25).astype(jnp.bfloat16)
    latents = gather_rows(gather_rows(my_latents, groups.high, 7), groups.low, 8)
    row_scale = row_count ** (-0.5)
    recon = jnp.dot(latents, dec_weight, preferred_element_type=jnp.float32)
    recon = scatter_sum(recon.astype(jnp.bfloat16), groups.shards, 9)
    piece_len = recon.shape[0]
    target = lax.dynamic_slice_in_dim(block, shard_pos * piece_len, piece_len, 0).astype(
        jnp.float32
    )
    scaled_error = ((recon + dec_bias - target) * row_scale).astype(jnp.bfloat16)
    error_all = gather_rows(scaled_error, groups.shards, 10)
    dec_bias_grad = jnp.sum(error_all, axis=0, dtype=jnp.float32)
    latent_part = lax.dot_general(
        error_all, dec_weight, (((1,), (1,)), ((), ())), preferred_element_type=jnp.float32
    )
    dec_grad = lax.dot_general(
        latents, error_all, (((0,), (0,)), ((), ())), preferred_element_type=jnp.float32
    )
    latent_grad = scatter_sum(latent_part.astype(jnp.bfloat16), groups.low, 11).astype(jnp.bfloat16)
    latent_grad = scatter_sum(latent_grad, groups.high, 12)
    my_grad = (latent_grad * jax.nn.sigmoid(4.0 * preact)).astype(jnp.bfloat16)
    preact_grad = gather_rows(gather_rows(my_grad, groups.high, 13), groups.low, 14)
    enc_grad = lax.dot_general(
        block, preact_grad, (((0,), (0,)), ((), ())), preferred_element_type=jnp.float32
    ).astype(jnp.bfloat16)
    enc_bias_grad = jnp.sum(preact_grad, axis=0, dtype=jnp.float32)
    return (layer_out, enc_grad, enc_bias_grad, dec_grad.astype(jnp.bfloat16), dec_bias_grad)


def solution(mesh):
    placed = (
        P(None, "wid", None),
        P(None, ("grp", "ctx"), "wid", None),
        P(None, ("grp", "ctx"), "wid", None),
        P(),
        P(),
        P("wid", ("grp", "ctx")),
        P("wid", ("grp", "ctx")),
        P("wid", ("grp", "ctx")),
        P(("grp", "ctx")),
        P(("grp", "ctx"), "wid"),
        P("wid"),
    )
    return jax.shard_map(
        functools.partial(body, dict(mesh.shape)),
        mesh=mesh,
        in_specs=placed,
        out_specs=(
            P("wid", ("grp", "ctx")),
            P("wid", ("grp", "ctx")),
            P(("grp", "ctx")),
            P(("grp", "ctx"), "wid"),
            P("wid"),
        ),
        check_vma=False,
    )
```

```python
import functools

import jax
import jax.numpy as jnp
from jax import lax
from jax.experimental import pallas as pl
from jax.experimental.pallas import tpu as pltpu
from jax.sharding import PartitionSpec as P

HD = 128
MESH = pl.DeviceIdType.MESH


def exchange_kernel(n, where, peer_id, gather, x_ref, out_ref, send_sem, recv_sem):
    me = where()
    peers = [lax.rem(me + step, n) for step in range(1, n)]
    barrier = pltpu.get_barrier_semaphore()
    for peer in peers:
        pl.semaphore_signal(barrier, inc=1, device_id=peer_id(peer), device_id_type=MESH)
    pl.semaphore_wait(barrier, n - 1)

    def copy_to(step, peer):
        return pltpu.make_async_remote_copy(
            src_ref=x_ref if gather else x_ref.at[peer],
            dst_ref=out_ref.at[me],
            send_sem=send_sem.at[step],
            recv_sem=recv_sem.at[me],
            device_id=peer_id(peer),
            device_id_type=MESH,
        )

    def copy_from(step, peer):
        return pltpu.make_async_remote_copy(
            src_ref=x_ref if gather else x_ref.at[peer],
            dst_ref=out_ref.at[peer],
            send_sem=send_sem.at[step],
            recv_sem=recv_sem.at[peer],
            device_id=peer_id(peer),
            device_id_type=MESH,
        )

    sends = [copy_to(step, peer) for step, peer in enumerate(peers)]
    for copy in sends:
        copy.start()
    out_ref[me] = x_ref[...] if gather else x_ref[me]
    for step, peer in enumerate(peers):
        copy_from(step, peer).wait_recv()
    for copy in sends:
        copy.wait_send()


def exchange(x, n, where, peer_id, gather, number):
    block = x.shape if gather else x.shape[1:]
    return pl.pallas_call(
        functools.partial(exchange_kernel, n, where, peer_id, gather),
        out_shape=jax.ShapeDtypeStruct((n,) + block, x.dtype),
        in_specs=[pl.BlockSpec(memory_space=pltpu.VMEM)],
        out_specs=pl.BlockSpec(memory_space=pltpu.VMEM),
        scratch_shapes=[pltpu.SemaphoreType.DMA((n,)), pltpu.SemaphoreType.DMA((n,))],
        compiler_params=pltpu.CompilerParams(
            collective_id=number, has_side_effects=True, vmem_limit_bytes=24 * 1024 * 1024
        ),
        name="exchange%d" % number,
    )(x)


class Groups:
    def __init__(self, sizes):
        ctx_n = sizes["ctx"]
        self.shards = (
            sizes["grp"] * ctx_n,
            lambda: lax.axis_index("grp") * ctx_n + lax.axis_index("ctx"),
            lambda p: {"grp": p // ctx_n, "ctx": lax.rem(p, ctx_n)},
        )
        self.wid = (sizes["wid"], lambda: lax.axis_index("wid"), lambda p: {"wid": p})
        self.low = (
            2,
            lambda: lax.rem(lax.axis_index("wid"), 2),
            lambda p: {"wid": (lax.axis_index("wid") // 2) * 2 + p},
        )
        self.high = (
            sizes["wid"] // 2,
            lambda: lax.axis_index("wid") // 2,
            lambda p: {"wid": p * 2 + lax.rem(lax.axis_index("wid"), 2)},
        )


def scatter_sum(x, group, number):
    n = group[0]
    parts = exchange(x.reshape((n, x.shape[0] // n) + x.shape[1:]), *group, False, number)
    return jnp.sum(parts.astype(jnp.float32), axis=0)


def gather_rows(x, group, number):
    whole = exchange(x, *group, True, number)
    return whole.reshape((whole.shape[0] * whole.shape[1],) + whole.shape[2:])


def rows_at(start, size):
    return pl.ds(pl.multiple_of(start, 16), size)


def cols_at(start, size):
    return pl.ds(pl.multiple_of(start, 128), size)


def partners(me, n):
    if n == 2:
        to = [1 - me]
        return to, to
    if n == 4:
        near = me + 1 - 2 * lax.rem(me, 2)
        to = [near, lax.rem(me + 2, 4), lax.rem(near + 2, 4)]
        return to, to
    return (
        [lax.rem(me + k, n) for k in range(1, n)],
        [lax.rem(me + n - k, n) for k in range(1, n)],
    )


class Plan:
    def __init__(self, sizes, query, keys, resid, enc_weight):
        self.grp, self.ctx, self.wid = sizes["grp"], sizes["ctx"], sizes["wid"]
        self.high = self.wid // 2
        self.shards = self.grp * self.ctx
        self.row_count, self.heads_local, self.head_dim = query.shape
        self.seqs, self.slots, self.kv_local = keys.shape[:3]
        self.heads = self.heads_local // self.kv_local
        self.width, self.latents = enc_weight.shape
        self.cols = resid.shape[1]
        self.streams = 2
        self.rows = self.row_count // self.streams
        self.half = self.rows // 2
        self.quarter = self.rows // self.wid
        self.side = self.rows // self.ctx
        self.piece = self.side // self.grp
        self.cuts = 2

    def fits(self):
        return (
            self.wid % 2 == 0
            and self.grp == self.wid == self.seqs
            and self.ctx == self.kv_local
            and self.ctx > 1
            and self.rows % (16 * self.wid) == 0
            and self.rows % (16 * self.shards) == 0
            and self.cols % 128 == 0
            and self.cols * self.ctx == self.width
            and self.width % (128 * self.cuts) == 0
            and self.latents % 1024 == 0
            and self.head_dim % 128 == 0
            and self.heads % 2 == 0
        )


def fused_kernel(
    plan, query, cache, len_hbm, pos_hbm, resid_hbm, eb_hbm, db_hbm, out_hbm, enc_hbm, dec_hbm,
    layer_out, block_t, dec_grad, dec_sum, pgrad,
    lat_t, err, lengths, query_pos, resid, enc_bias, dec_bias, out_w, enc_w, dec_w, kv, att, proj, opair_in, opair_sum, ohigh_in, zin, block, lat,
    part, pair_in, pair_sum, high_in, factor, recon, side_in, side_sum, piece_in,
    load_sem, kv_sem, att_sem, att_cross, opair_sem, ohigh_sem, lo_sem, blk_sem, blk_cross,
    pair_sem, high_sem, gather_sem, relay_sem, side_sem, piece_sem, spread_sem, cross_sem,
):
    p = plan
    g, c, w = lax.axis_index("grp"), lax.axis_index("ctx"), lax.axis_index("wid")
    low, high = lax.rem(w, 2), w // 2
    partner = {"wid": w + 1 - 2 * low}
    highs, highs_from = partners(high, p.high)
    ctxs, ctxs_from = partners(c, p.ctx)
    grps, grps_from = partners(g, p.grp)
    to_high = lambda h: {"wid": h * 2 + low}
    to_ctx = lambda q: {"ctx": q}
    to_grp = lambda q: {"grp": q}
    others = [(1 - low, high)] + [(low, h) for h in highs_from] + [(1 - low, h) for h in highs_from]
    shard_to = [(q, r) for q in [g] + grps for r in [c] + ctxs][1:]
    shard_from = [(q, r) for q in [g] + grps_from for r in [c] + ctxs_from][1:]

    enc_step = 512
    enc_steps = p.latents // enc_step

    def load(src, dst, index):
        copy = pltpu.make_async_copy(src, dst, load_sem.at[index])
        copy.start()
        return copy

    barrier = pltpu.get_barrier_semaphore()
    greeted = [{"grp": q, "ctx": r} for q, r in shard_to]
    greeted += [{"wid": hi * 2 + lo} for lo, hi in others]
    for peer in greeted:
        pl.semaphore_signal(barrier, inc=1, device_id=peer, device_id_type=MESH)
    small_loads = [
        load(src, dst, 3 + k)
        for k, (src, dst) in enumerate(
            [(len_hbm, lengths), (pos_hbm, query_pos), (resid_hbm, resid), (eb_hbm, enc_bias), (db_hbm, dec_bias)]
        )
    ]
    out_load = load(out_hbm, out_w, 0)
    enc_load = load(enc_hbm, enc_w, 1)
    dec_load = load(dec_hbm, dec_w, 2)
    pl.semaphore_wait(barrier, len(greeted))

    pending = []

    def send(src, dst, sem, index, peer, to_index=None, when=None):
        copy = pltpu.make_async_remote_copy(
            src_ref=src, dst_ref=dst, send_sem=sem.at[(0,) + index],
            recv_sem=sem.at[(1,) + (index if to_index is None else to_index)],
            device_id=peer, device_id_type=MESH,
        )
        if when is None:
            copy.start()
        else:
            pl.when(when)(lambda: copy.start())
        pending.append((copy, when))

    def arrived(ref, sem, index):
        pltpu.make_async_remote_copy(
            src_ref=ref, dst_ref=ref, send_sem=sem.at[(0,) + index], recv_sem=sem.at[(1,) + index],
            device_id=partner, device_id_type=MESH,
        ).wait_recv()

    def quarter_row(t, lo, hi):
        return t * p.rows + (lo * p.high + hi) * p.quarter

    def piece_row(t, q, r):
        return t * p.rows + q * p.side + r * p.piece

    def shard(q, r):
        return q * p.ctx + r

    def loop(count, body):
        def step(i, carry):
            body(pl.multiple_of(i * 16, 16))
            return carry

        lax.fori_loop(0, count // 16, step, 0)

    def cache_send():
        for k, (q, r) in reversed(list(enumerate(shard_to))):
            send(
                cache.at[shard(q, r)], kv.at[rows_at(shard(g, c) * p.slots, p.slots)],
                kv_sem, (k,), {"grp": q, "ctx": r},
            )
        kv[rows_at(shard(g, c) * p.slots, p.slots)] = cache[shard(g, c)]

    def cache_wait():
        for k, (q, r) in enumerate(shard_from):
            arrived(kv.at[rows_at(shard(q, r) * p.slots, p.slots)], kv_sem, (k,))

    def att_at(t, q, r):
        return att.at[
            rows_at(quarter_row(t, lax.rem(q, 2), q // 2), p.quarter),
            cols_at(r * p.heads * p.head_dim, p.heads * p.head_dim),
        ]

    def key_positions():
        live = lengths[pl.ds(g, 1), :]
        slot = lax.broadcasted_iota(jnp.int32, (1, p.shards * p.slots), 1)
        key = jnp.full((1, p.shards * p.slots), 2**30, jnp.int32)
        offset = jnp.zeros((1, 1), jnp.int32)
        for b in range(p.shards):
            count = live[:, b : b + 1]
            own = slot - b * p.slots
            key = jnp.where((own >= 0) & (own < p.slots) & (own < count), offset + own, key)
            offset = offset + count
        return key

    def row_positions(t):
        shape = (2 * p.quarter, p.row_count)
        row = lax.broadcasted_iota(jnp.int32, shape, 0)
        wanted = lax.rem(row, p.quarter) + (g * (p.row_count // p.seqs) + t * p.quarter)
        here = lax.broadcasted_iota(jnp.int32, shape, 1) == wanted
        values = jnp.where(here, query_pos[...].reshape(1, -1).astype(jnp.float32), 0.0)
        return jnp.sum(values, axis=1, keepdims=True).astype(jnp.int32)

    def attend_rows(t):
        two = 2 * p.quarter
        visible = key_positions() <= row_positions(t)
        mine = att_at(t, g, c)
        for i in range(p.heads // 2):
            scores = lax.dot_general(
                query[t, pl.ds(i * two, two)], kv[:, : p.head_dim], (((1,), (1,)), ((), ())),
                preferred_element_type=jnp.float32,
            ) * p.head_dim ** (-0.5)
            peak = jnp.max(jnp.where(visible, scores, -1e30), axis=-1, keepdims=True)
            weights = jnp.where(visible, jnp.exp(scores - peak), 0.0)
            total = jnp.sum(weights, axis=-1, keepdims=True)
            weighted = jnp.dot(
                weights.astype(jnp.bfloat16), kv[:, p.head_dim :], preferred_element_type=jnp.float32
            )
            out = (weighted / total).astype(jnp.bfloat16)
            for j in range(2):
                mine[:, pl.ds((2 * i + j) * p.head_dim, p.head_dim)] = out[j * p.quarter : (j + 1) * p.quarter]
        for k, q in enumerate(grps):
            send(mine, mine, att_sem, (t, k), to_grp(q))
        for i, r in enumerate(ctxs):
            send(mine, mine, att_cross, (t, i, 0), to_ctx(r))

    def att_relay(t):
        for k, q in enumerate(grps_from):
            theirs = att_at(t, q, c)
            arrived(theirs, att_sem, (t, k))
            for i, r in enumerate(ctxs):
                send(theirs, theirs, att_cross, (t, i, k + 1), to_ctx(r))

    def project(t):
        for i, r in enumerate(ctxs_from):
            for k, q in enumerate([g] + grps_from):
                arrived(att_at(t, q, r), att_cross, (t, i, k))
        if t == 0:
            out_load.wait()
        rows = pl.ds(t * p.rows, p.rows)
        proj[rows] = jnp.dot(att[rows], out_w[...], preferred_element_type=jnp.float32).astype(jnp.bfloat16)
        send(
            proj.at[rows_at(t * p.rows + (1 - low) * p.half, p.half)], opair_in.at[t], opair_sem, (t,), partner
        )

    def project_add(t):
        arrived(opair_in.at[t], opair_sem, (t,))

        def body(r):
            mine = proj[rows_at(t * p.rows + low * p.half + r, 16)].astype(jnp.float32)
            opair_sum[t, pl.ds(r, 16)] = (mine + opair_in[t, pl.ds(r, 16)].astype(jnp.float32)).astype(jnp.bfloat16)

        loop(p.half, body)
        for s, h in enumerate(highs):
            send(opair_sum.at[t, rows_at(h * p.quarter, p.quarter)], ohigh_in.at[t, s], ohigh_sem, (t, s), to_high(h))

    def layer(t):
        for s in range(len(highs)):
            arrived(ohigh_in.at[t, s], ohigh_sem, (t, s))

        def body(r):
            total = opair_sum[t, rows_at(high * p.quarter + r, 16)].astype(jnp.float32)
            for s in range(len(highs)):
                total = total + ohigh_in[t, s, pl.ds(r, 16)].astype(jnp.float32)
            rows = rows_at(t * p.quarter + r, 16)
            value = (total + resid[rows].astype(jnp.float32)).astype(jnp.bfloat16)
            layer_out[rows] = value
            zin[t, g, pl.ds(r, 16)] = value

        loop(p.quarter, body)
        for k, q in enumerate(grps):
            send(zin.at[t, g], zin.at[t, g], lo_sem, (t, k), to_grp(q))

    def block_at(t, lo, hi, r):
        return block.at[rows_at(quarter_row(t, lo, hi), p.quarter), cols_at(r * p.cols, p.cols)]

    def block_relay(t):
        mine = block_at(t, low, high, c)
        for k, q in enumerate([g] + grps_from):
            if k:
                arrived(zin.at[t, q], lo_sem, (t, k - 1))
            owned, away = w == q, w != q

            @pl.when(owned)
            def _(q=q):
                mine[...] = zin[t, q]

            for i, r in enumerate(ctxs):
                send(mine, mine, blk_cross, (t, i, 0, k), to_ctx(r), (t, i, 0, 0), owned)
            send(zin.at[t, q], mine, blk_sem, (t, k), {"wid": q}, (t, w), away)

    def block_spread(t):
        for j, (lo, hi) in enumerate(others):
            theirs = block_at(t, lo, hi, c)
            arrived(theirs, blk_sem, (t, hi * 2 + lo))
            for i, r in enumerate(ctxs):
                send(theirs, theirs, blk_cross, (t, i, j + 1, 0), to_ctx(r))

    def block_wait(t):
        for i, r in enumerate(ctxs_from):
            for j, (lo, hi) in enumerate([(low, high)] + others):
                arrived(block_at(t, lo, hi, r), blk_cross, (t, i, j, 0))

    lat_half = p.latents // 2
    spans = [(u, pl.ds(u * lat_half, lat_half)) for u in range(2)]

    def pair_send(k, t, u, cols):
        there = part.at[k, rows_at(t * p.rows + (1 - low) * p.half, p.half), cols]
        send(there, pair_in.at[k, t, :, cols], pair_sem, (k, t, u), partner)

    def pair_add(k, t):
        for u, cols in spans:
            arrived(pair_in.at[k, t, :, cols], pair_sem, (k, t, u))

            def body(r, cols=cols):
                mine = part[k, rows_at(t * p.rows + low * p.half + r, 16), cols].astype(jnp.float32)
                theirs = pair_in[k, t, pl.ds(r, 16), cols].astype(jnp.float32)
                pair_sum[k, t, pl.ds(r, 16), cols] = (mine + theirs).astype(jnp.bfloat16)

            loop(p.half, body)
            for s, h in enumerate(highs):
                send(
                    pair_sum.at[k, t, rows_at(h * p.quarter, p.quarter), cols], high_in.at[k, t, s, :, cols],
                    high_sem, (k, t, u, s), to_high(h),
                )

    def high_sum(k, t, r, cols):
        total = pair_sum[k, t, rows_at(high * p.quarter + r, 16), cols].astype(jnp.float32)
        for s in range(len(highs)):
            total = total + high_in[k, t, s, pl.ds(r, 16), cols].astype(jnp.float32)
        return total

    def high_wait(k, t, u, cols):
        for s in range(len(highs)):
            arrived(high_in.at[k, t, s, :, cols], high_sem, (k, t, u, s))

    def publish(k, t, u, cols, out):
        mine = out.at[rows_at(quarter_row(t, low, high), p.quarter), cols]
        for s, h in enumerate(highs):
            send(mine, mine, gather_sem, (k, t, u, s + 1), to_high(h))
        send(mine, mine, gather_sem, (k, t, u, 0), partner)

    def activate(t):
        for u, cols in spans:
            high_wait(0, t, u, cols)

            def body(r, cols=cols):
                z = 4.0 * (high_sum(0, t, r, cols) + enc_bias[cols].reshape(1, -1))
                e = jnp.exp(-jnp.abs(z))
                lat[rows_at(quarter_row(t, low, high) + r, 16), cols] = (
                    (jnp.maximum(z, 0.0) + jnp.log1p(e)) * 0.25
                ).astype(jnp.bfloat16)
                factor[t, pl.ds(r, 16), cols] = jnp.where(z >= 0.0, 1.0, e) / (1.0 + e)

            loop(p.quarter, body)
            publish(0, t, u, cols, lat)

    def cotangent(t):
        for u, cols in spans:
            high_wait(1, t, u, cols)

            def body(r, cols=cols):
                pgrad[rows_at(quarter_row(t, low, high) + r, 16), cols] = (
                    high_sum(1, t, r, cols) * factor[t, pl.ds(r, 16), cols]
                ).astype(jnp.bfloat16)

            loop(p.quarter, body)
            publish(1, t, u, cols, pgrad)

    def relay(k, t, out):
        for u, cols in spans:
            for s, h in enumerate(highs_from):
                theirs = out.at[rows_at(quarter_row(t, low, h), p.quarter), cols]
                arrived(theirs, gather_sem, (k, t, u, s + 1))
                send(theirs, theirs, relay_sem, (k, t, u, s), partner)

    def collected(k, t, out):
        for u, cols in spans:
            arrived(out.at[rows_at(quarter_row(t, 1 - low, high), p.quarter), cols], gather_sem, (k, t, u, 0))
            for s, h in enumerate(highs_from):
                arrived(out.at[rows_at(quarter_row(t, 1 - low, h), p.quarter), cols], relay_sem, (k, t, u, s))

    def encode(t):
        block_wait(t)
        if t == 0:
            enc_load.wait()
        rows = pl.ds(t * p.rows, p.rows)

        def step(j, carry):
            cols = cols_at(j * enc_step, enc_step)
            part[0, rows, cols] = jnp.dot(
                block[rows, :], enc_w[:, cols], preferred_element_type=jnp.float32
            ).astype(jnp.bfloat16)
            return carry

        for u, cols in spans:
            lax.fori_loop(u * enc_steps // 2, (u + 1) * enc_steps // 2, step, 0)
            pair_send(0, t, u, cols)

    cut = p.width // p.cuts

    def decode(t):
        collected(0, t, lat)
        if t == 0:
            dec_load.wait()
        rows = pl.ds(t * p.rows, p.rows)
        for j in range(p.cuts):
            cols = pl.ds(j * cut, cut)
            recon[rows, cols] = jnp.dot(
                lat[rows, :], dec_w[:, cols], preferred_element_type=jnp.float32
            ).astype(jnp.bfloat16)
            for s, q in enumerate(ctxs):
                send(
                    recon.at[rows_at(piece_row(t, q, 0), p.side), cols], side_in.at[t, s, :, cols],
                    side_sem, (t, j, s), to_ctx(q),
                )

    def side_add(t):
        for j in range(p.cuts):
            cols = pl.ds(j * cut, cut)
            for s in range(len(ctxs)):
                arrived(side_in.at[t, s, :, cols], side_sem, (t, j, s))
            total = recon[rows_at(piece_row(t, c, 0), p.side), cols].astype(jnp.float32)
            for s in range(len(ctxs)):
                total = total + side_in[t, s, :, cols].astype(jnp.float32)
            side_sum[t, :, cols] = total.astype(jnp.bfloat16)
            for s, q in enumerate(grps):
                send(
                    side_sum.at[t, rows_at(q * p.piece, p.piece), cols], piece_in.at[t, s, :, cols],
                    piece_sem, (t, j, s), to_grp(q),
                )

    def err_at(t, q, r, cols):
        return err.at[rows_at(piece_row(t, q, r), p.piece), cols]

    def error(t):
        for j in range(p.cuts):
            cols = pl.ds(j * cut, cut)
            for s in range(len(grps)):
                arrived(piece_in.at[t, s, :, cols], piece_sem, (t, j, s))
            total = side_sum[t, rows_at(g * p.piece, p.piece), cols].astype(jnp.float32)
            for s in range(len(grps)):
                total = total + piece_in[t, s, :, cols].astype(jnp.float32)
            rows = rows_at(piece_row(t, c, g), p.piece)
            wanted = block[rows, cols].astype(jnp.float32)
            err[rows, cols] = ((total + dec_bias[cols].reshape(1, -1) - wanted) * p.row_count ** (-0.5)).astype(jnp.bfloat16)
            mine = err_at(t, c, g, cols)
            for s, q in enumerate(grps):
                send(mine, mine, spread_sem, (t, j, s), to_grp(q))
            for s, q in enumerate(ctxs):
                send(mine, mine, cross_sem, (t, j, s, 0), to_ctx(q))

    def error_relay(t):
        for j in range(p.cuts):
            cols = pl.ds(j * cut, cut)
            for i, r in enumerate(grps_from):
                theirs = err_at(t, c, r, cols)
                arrived(theirs, spread_sem, (t, j, i))
                for s, q in enumerate(ctxs):
                    send(theirs, theirs, cross_sem, (t, j, s, i + 1), to_ctx(q))

    def back(t):
        for j in range(p.cuts):
            for s, q in enumerate(ctxs_from):
                for i, r in enumerate([g] + grps_from):
                    arrived(err_at(t, q, r, pl.ds(j * cut, cut)), cross_sem, (t, j, s, i))
        rows = pl.ds(t * p.rows, p.rows)

        def step(j, carry):
            cols = pl.ds(pl.multiple_of(j * enc_step, enc_step), enc_step)
            part[1, rows, cols] = lax.dot_general(
                err[rows, :], dec_w[cols, :], (((1,), (1,)), ((), ())), preferred_element_type=jnp.float32
            ).astype(jnp.bfloat16)
            return carry

        for u, cols in spans:
            lax.fori_loop(u * enc_steps // 2, (u + 1) * enc_steps // 2, step, 0)
            pair_send(1, t, u, cols)

    out_step = 512

    def outer(j):
        rows = pl.ds(j * out_step, out_step)
        dec_grad[rows] = jnp.dot(lat_t[rows, :], err[...], preferred_element_type=jnp.float32).astype(jnp.bfloat16)

    def error_sum():
        dec_sum[...] = jnp.sum(err[...].astype(jnp.float32), axis=0)

    def outers(first, last):
        for j in range(first * (p.latents // out_step) // 6, last * (p.latents // out_step) // 6):
            outer(j)

    def turn(src, dst, t, count):
        rows = pl.ds(t * p.rows, p.rows)

        def step(j, carry):
            cols = cols_at(j * 256, 256)
            dst[cols, rows] = src[rows, cols].T
            return carry

        lax.fori_loop(0, count // 256, step, 0)

    cache_send()
    for copy in small_loads:
        copy.wait()
    cache_wait()
    stages = [
        lambda: attend_rows(0),
        lambda: attend_rows(1),
        lambda: att_relay(0),
        lambda: project(0),
        lambda: att_relay(1),
        lambda: project_add(0),
        lambda: project(1),
        lambda: layer(0),
        lambda: project_add(1),
        lambda: block_relay(0),
        lambda: layer(1),
        lambda: block_spread(0),
        lambda: block_relay(1),
        lambda: block_spread(1),
        lambda: encode(0),
        lambda: pair_add(0, 0),
        lambda: encode(1),
        lambda: pair_add(0, 1),
        lambda: turn(block, block_t, 0, p.width),
        lambda: turn(block, block_t, 1, p.width),
        lambda: activate(0),
        lambda: activate(1),
        lambda: relay(0, 0, lat),
        lambda: decode(0),
        lambda: turn(lat, lat_t, 0, p.latents),
        lambda: relay(0, 1, lat),
        lambda: side_add(0),
        lambda: decode(1),
        lambda: error(0),
        lambda: side_add(1),
        lambda: turn(lat, lat_t, 1, p.latents),
        lambda: error_relay(0),
        lambda: error(1),
        lambda: back(0),
        lambda: error_relay(1),
        lambda: pair_add(1, 0),
        lambda: back(1),
        lambda: pair_add(1, 1),
        lambda: cotangent(0),
        lambda: outers(0, 3),
        lambda: cotangent(1),
        lambda: outers(3, 6),
        error_sum,
        lambda: relay(1, 0, pgrad),
        lambda: relay(1, 1, pgrad),
        lambda: collected(1, 0, pgrad),
        lambda: collected(1, 1, pgrad),
    ]
    for stage in stages:
        stage()
    for copy, when in pending:
        if when is None:
            copy.wait_send()
        else:
            pl.when(when)(lambda copy=copy: copy.wait_send())


def fused(plan, query, keys, values, lengths, query_pos, resid, out_weight, enc_weight, enc_bias, dec_weight, dec_bias):
    p = plan
    low = jnp.bfloat16
    g, c = lax.axis_index("grp"), lax.axis_index("ctx")
    cache = jnp.concatenate([keys, values], axis=-1).transpose(0, 2, 1, 3)
    cache = cache.reshape(p.shards, p.slots, 2 * p.head_dim)
    seq_rows = p.row_count // p.seqs
    mine = lax.dynamic_slice(query, (g * seq_rows, c * p.heads, 0), (seq_rows, p.heads, p.head_dim))
    mine = mine.reshape(p.streams, p.quarter, p.heads, p.head_dim).transpose(0, 2, 1, 3)
    mine = mine.reshape(p.streams, p.heads * p.quarter, p.head_dim)

    vmem = pl.BlockSpec(memory_space=pltpu.VMEM)
    hbm = pl.BlockSpec(memory_space=pltpu.HBM)
    n, highs, ctxs, grps = p.streams, p.high - 1, p.ctx - 1, p.grp - 1
    dma = pltpu.SemaphoreType.DMA
    return pl.pallas_call(
        functools.partial(fused_kernel, p),
        out_shape=(
            jax.ShapeDtypeStruct((n * p.quarter, p.cols), low),
            jax.ShapeDtypeStruct((p.width, p.row_count), low),
            jax.ShapeDtypeStruct((p.latents, p.width), low),
            jax.ShapeDtypeStruct((p.width,), jnp.float32),
            jax.ShapeDtypeStruct((p.row_count, p.latents), low),
        ),
        in_specs=[vmem] * 2 + [hbm] * 8,
        out_specs=(vmem,) * 5,
        scratch_shapes=[
            pltpu.VMEM((p.latents, p.row_count), low),
            pltpu.VMEM((p.row_count, p.width), low),
            pltpu.VMEM(lengths.shape, jnp.int32),
            pltpu.VMEM(query_pos.shape, jnp.int32),
            pltpu.VMEM(resid.shape, low),
            pltpu.VMEM(enc_bias.shape, jnp.float32),
            pltpu.VMEM(dec_bias.shape, jnp.float32),
            pltpu.VMEM(out_weight.shape, low),
            pltpu.VMEM((p.width, p.latents), low),
            pltpu.VMEM((p.latents, p.width), low),
            pltpu.VMEM((p.shards * p.slots, 2 * p.head_dim), low),
            pltpu.VMEM((p.row_count, p.heads_local * p.head_dim), low),
            pltpu.VMEM((p.row_count, p.cols), low),
            pltpu.VMEM((n, p.half, p.cols), low),
            pltpu.VMEM((n, p.half, p.cols), low),
            pltpu.VMEM((n, highs, p.quarter, p.cols), low),
            pltpu.VMEM((n, p.grp, p.quarter, p.cols), low),
            pltpu.VMEM((p.row_count, p.width), low),
            pltpu.VMEM((p.row_count, p.latents), low),
            pltpu.VMEM((2, p.row_count, p.latents), low),
            pltpu.VMEM((2, n, p.half, p.latents), low),
            pltpu.VMEM((2, n, p.half, p.latents), low),
            pltpu.VMEM((2, n, highs, p.quarter, p.latents), low),
            pltpu.VMEM((n, p.quarter, p.latents), jnp.float32),
            pltpu.VMEM((p.row_count, p.width), low),
            pltpu.VMEM((n, ctxs, p.side, p.width), low),
            pltpu.VMEM((n, p.side, p.width), low),
            pltpu.VMEM((n, grps, p.piece, p.width), low),
            dma((8,)),
            dma((2, p.shards - 1)),
            dma((2, n, grps)),
            dma((2, n, ctxs, grps + 1)),
            dma((2, n)),
            dma((2, n, highs)),
            dma((2, n, grps)),
            dma((2, n, p.grp)),
            dma((2, n, ctxs, p.wid, p.grp)),
            dma((2, 2, n, 2)),
            dma((2, 2, n, 2, highs)),
            dma((2, 2, n, 2, highs + 1)),
            dma((2, 2, n, 2, highs)),
            dma((2, n, p.cuts, ctxs)),
            dma((2, n, p.cuts, grps)),
            dma((2, n, p.cuts, grps)),
            dma((2, n, p.cuts, ctxs, grps + 1)),
        ],
        compiler_params=pltpu.CompilerParams(
            collective_id=0, has_side_effects=True, vmem_limit_bytes=40 * 1024 * 1024
        ),
        name="fused",
    )(
        mine, cache,
        *(
            pltpu.with_memory_space_constraint(x, pltpu.HBM)
            for x in (lengths, query_pos, resid, enc_bias, dec_bias, out_weight, enc_weight, dec_weight)
        ),
    )


def grads_kernel(
    step, depth, block_t, dec_in, dec_sum_in, pgrad, layer_in, enc_out, dec_out, enc_sum, dec_sum, layer_out, buf, sem, dec_sem,
):
    dec_rows = dec_in.shape[0] // 2
    halves = [
        pltpu.make_async_copy(
            dec_in.at[pl.ds(i * dec_rows, dec_rows)], dec_out.at[pl.ds(i * dec_rows, dec_rows)], dec_sem.at[i]
        )
        for i in range(2)
    ]
    for copy in halves:
        copy.start()
    count = enc_out.shape[0] // step
    started = []
    for i in range(count):
        slot = i % depth
        if i >= depth:
            started[i - depth].wait()
        rows = pl.ds(i * step, step)
        buf[slot] = jnp.dot(block_t[rows, :], pgrad[...], preferred_element_type=jnp.float32).astype(jnp.bfloat16)
        copy = pltpu.make_async_copy(buf.at[slot], enc_out.at[rows], sem.at[slot])
        copy.start()
        started.append(copy)
    layer_out[...] = layer_in[...]
    dec_sum[...] = dec_sum_in[...]
    enc_sum[...] = jnp.sum(pgrad[...].astype(jnp.float32), axis=0)
    for copy in started[max(0, count - depth) :] + halves:
        copy.wait()


def grads(block_t, dec_grad, dec_bias_grad, pgrad, layer_in):
    width, latents = block_t.shape[0], pgrad.shape[1]
    vmem = pl.BlockSpec(memory_space=pltpu.VMEM)
    hbm = pl.BlockSpec(memory_space=pltpu.HBM)
    step, depth = 256, 5
    enc, dec, enc_sum, dec_sum, layer_out = pl.pallas_call(
        functools.partial(grads_kernel, step, depth),
        out_shape=(
            jax.ShapeDtypeStruct((width, latents), jnp.bfloat16),
            jax.ShapeDtypeStruct((latents, width), jnp.bfloat16),
            jax.ShapeDtypeStruct((latents,), jnp.float32),
            jax.ShapeDtypeStruct((width,), jnp.float32),
            jax.ShapeDtypeStruct(layer_in.shape, layer_in.dtype),
        ),
        in_specs=[vmem] * 5,
        out_specs=(hbm, hbm, vmem, vmem, vmem),
        scratch_shapes=[
            pltpu.VMEM((depth, step, latents), jnp.bfloat16),
            pltpu.SemaphoreType.DMA((depth,)),
            pltpu.SemaphoreType.DMA((2,)),
        ],
        compiler_params=pltpu.CompilerParams(vmem_limit_bytes=16 * 1024 * 1024),
        name="grads",
    )(block_t, dec_grad, dec_bias_grad, pgrad, layer_in)
    return layer_out, enc, enc_sum, dec, dec_sum


def attend(groups, query, keys, values, lengths, query_pos):
    seq_count, slot_count, kv_local, head_dim = keys.shape
    row_count, heads_local = query.shape[:2]
    group_size = heads_local // kv_local
    shards = groups.shards[0]
    pairs = seq_count * kv_local
    chunks = shards // pairs
    rows = row_count // seq_count // chunks
    pair = lax.axis_index(("grp", "ctx")) // chunks
    seq, head = pair // kv_local, lax.rem(pair, kv_local)
    row0 = seq * (row_count // seq_count) + lax.rem(lax.axis_index(("grp", "ctx")), chunks) * rows
    cache = jnp.concatenate([keys, values], axis=-1).transpose(0, 2, 1, 3)
    cache = cache.reshape(pairs, slot_count, 2 * head_dim)
    if chunks > 1:
        cache = jnp.repeat(cache, chunks, axis=0)
    cache = exchange(cache, *groups.shards, False, 0).reshape(shards * slot_count, 2 * head_dim)
    q = lax.dynamic_slice(query, (row0, head * group_size, 0), (rows, group_size, head_dim))
    live = lax.dynamic_index_in_dim(lengths, seq, 0, keepdims=False)
    before = jnp.arange(shards)[None, :] < jnp.arange(shards)[:, None]
    offset = jnp.sum(jnp.where(before, live[None, :], 0), axis=1)
    slot_ids = jnp.arange(slot_count, dtype=jnp.int32)
    key_pos = jnp.where(
        slot_ids[None, :] < live[:, None], offset[:, None] + slot_ids[None, :], jnp.int32(2**30)
    ).reshape(-1)
    position = lax.dynamic_slice_in_dim(query_pos, row0, rows, 0)
    visible = (key_pos[None, :] <= position[:, None])[:, None, :]
    scores = jnp.einsum(
        "rgd,td->rgt", q, cache[:, :head_dim], preferred_element_type=jnp.float32
    ) * HD ** (-0.5)
    peak = jnp.max(jnp.where(visible, scores, -1e30), axis=-1, keepdims=True)
    weights = jnp.where(visible, jnp.exp(scores - peak), 0.0)
    weight_sum = jnp.sum(weights, axis=-1, keepdims=True)
    weighted = jnp.einsum(
        "rgt,td->rgd", weights.astype(jnp.bfloat16), cache[:, head_dim:],
        preferred_element_type=jnp.float32,
    )
    mine = (weighted / weight_sum).astype(jnp.bfloat16).reshape(rows, group_size * head_dim)
    attention = exchange(mine, *groups.shards, True, 1)
    attention = attention.reshape(seq_count, kv_local, chunks, rows, group_size * head_dim)
    return attention.transpose(0, 2, 3, 1, 4).reshape(row_count, heads_local * head_dim)


def body(
    sizes,
    query,
    keys,
    values,
    lengths,
    query_pos,
    resid,
    out_weight,
    enc_weight,
    enc_bias,
    dec_weight,
    dec_bias,
):
    plan = Plan(sizes, query, keys, resid, enc_weight)
    if plan.fits():
        layer_out, block_t, dec_grad, dec_bias_grad, pgrad = fused(
            plan, query, keys, values, lengths, query_pos, resid, out_weight,
            enc_weight, enc_bias, dec_weight, dec_bias,
        )
        return grads(block_t, dec_grad, dec_bias_grad, pgrad, layer_out)
    groups = Groups(sizes)
    row_count = query.shape[0]
    shard_pos = lax.axis_index(("grp", "ctx"))
    attention = attend(groups, query, keys, values, lengths, query_pos)
    projected = jnp.dot(attention, out_weight, preferred_element_type=jnp.float32)
    mixed = scatter_sum(projected.astype(jnp.bfloat16), groups.wid, 2)
    layer_out = (mixed + resid.astype(jnp.float32)).astype(jnp.bfloat16)
    rows, cols = layer_out.shape
    wid_n = sizes["wid"]
    wide = exchange(layer_out, *groups.shards, True, 3)
    wide = wide.reshape(wid_n, -1, rows, cols).transpose(0, 2, 1, 3).reshape(wid_n, rows, -1)
    block = exchange(wide, *groups.wid, False, 4).reshape(row_count, -1)
    enc_part = jnp.dot(block, enc_weight, preferred_element_type=jnp.float32)
    preact = scatter_sum(enc_part.astype(jnp.bfloat16), groups.low, 5).astype(jnp.bfloat16)
    preact = scatter_sum(preact, groups.high, 6) + enc_bias
    my_latents = (jax.nn.softplus(4.0 * preact) * 0.25).astype(jnp.bfloat16)
    latents = gather_rows(gather_rows(my_latents, groups.high, 7), groups.low, 8)
    row_scale = row_count ** (-0.5)
    recon = jnp.dot(latents, dec_weight, preferred_element_type=jnp.float32)
    recon = scatter_sum(recon.astype(jnp.bfloat16), groups.shards, 9)
    piece_len = recon.shape[0]
    target = lax.dynamic_slice_in_dim(block, shard_pos * piece_len, piece_len, 0).astype(
        jnp.float32
    )
    scaled_error = ((recon + dec_bias - target) * row_scale).astype(jnp.bfloat16)
    error_all = gather_rows(scaled_error, groups.shards, 10)
    dec_bias_grad = jnp.sum(error_all, axis=0, dtype=jnp.float32)
    latent_part = lax.dot_general(
        error_all, dec_weight, (((1,), (1,)), ((), ())), preferred_element_type=jnp.float32
    )
    dec_grad = lax.dot_general(
        latents, error_all, (((0,), (0,)), ((), ())), preferred_element_type=jnp.float32
    )
    latent_grad = scatter_sum(latent_part.astype(jnp.bfloat16), groups.low, 11).astype(jnp.bfloat16)
    latent_grad = scatter_sum(latent_grad, groups.high, 12)
    my_grad = (latent_grad * jax.nn.sigmoid(4.0 * preact)).astype(jnp.bfloat16)
    preact_grad = gather_rows(gather_rows(my_grad, groups.high, 13), groups.low, 14)
    enc_grad = lax.dot_general(
        block, preact_grad, (((0,), (0,)), ((), ())), preferred_element_type=jnp.float32
    ).astype(jnp.bfloat16)
    enc_bias_grad = jnp.sum(preact_grad, axis=0, dtype=jnp.float32)
    return (layer_out, enc_grad, enc_bias_grad, dec_grad.astype(jnp.bfloat16), dec_bias_grad)


def solution(mesh):
    placed = (
        P(None, "wid", None),
        P(None, ("grp", "ctx"), "wid", None),
        P(None, ("grp", "ctx"), "wid", None),
        P(),
        P(),
        P("wid", ("grp", "ctx")),
        P("wid", ("grp", "ctx")),
        P("wid", ("grp", "ctx")),
        P(("grp", "ctx")),
        P(("grp", "ctx"), "wid"),
        P("wid"),
    )
    return jax.shard_map(
        functools.partial(body, dict(mesh.shape)),
        mesh=mesh,
        in_specs=placed,
        out_specs=(
            P("wid", ("grp", "ctx")),
            P("wid", ("grp", "ctx")),
            P(("grp", "ctx")),
            P(("grp", "ctx"), "wid"),
            P("wid"),
        ),
        check_vma=False,
    )
```
